32 devices in a mesh: dp: 4 (over x, y), tp: 8 (over z, core).
Axes of the slice: x: 2, y: 2, z: 4, core: 2. Of those that a mesh axis runs over, the one named last changes fastest.
Arguments:
- x_tokens: bfloat16 [4, 2048, 2560], P('dp', 'tp'), parts along dimension 0
- ln1_gain: float32 [2, 2560], replicated
- ln1_bias: float32 [2, 2560], replicated
- ln2_gain: float32 [2, 2560], replicated
- ln2_bias: float32 [2, 2560], replicated
- w_qkv: bfloat16 [2, 2560, 3, 32, 80], P(None, None, None, 'tp')
- w_out: bfloat16 [2, 32, 80, 2560], P(None, 'tp')
- b_out: float32 [2, 2560], replicated
- w_up: bfloat16 [2, 2560, 10240], P(None, None, 'tp')
- b_up: float32 [2, 10240], P(None, 'tp')
- w_down: bfloat16 [2, 10240, 2560], P(None, 'tp')
- b_down: float32 [2, 2560], replicated
Outputs:
- output: bfloat16 [4, 2048, 2560], P('dp', 'tp'), parts along dimension 0
There are 4 independent parts. The reference program is written for one: setup_inputs(seed, part) draws one part's arguments, and reference() takes and returns one part's arrays. A program takes and returns all parts, laid end to end along the dimension named above; an argument that names none is the same for every part.
All inputs are finite; a program needn't handle non-finite values.
Results may differ from the reference program's by a relative error of at most 0.0104064.
Values are sent between devices in bfloat16 or wider.
A program may use at most 1 GiB of HBM per device.

```python
import math
import jax
import jax.numpy as jnp
from jax import lax

BATCH = 1
SEQ_LEN = 2048
D_MODEL = 2560
HEADS = 32
HEAD_DIM = 80
D_FF = 10240
LAYERS = 2


def setup_inputs(seed: int = 0, part: int = 0) -> dict:
    base_key = jax.random.key(seed)
    part_key = jax.random.fold_in(base_key, part)
    row_key, tok_key = jax.random.split(part_key)
    keys = jax.random.split(base_key, 11)
    row_scale = 0.5 + jax.random.uniform(row_key, (BATCH, SEQ_LEN, 1), jnp.float32)
    tokens = jax.random.normal(tok_key, (BATCH, SEQ_LEN, D_MODEL), jnp.float32) * row_scale
    qk_gain = (math.log(SEQ_LEN) / 2.0) ** 0.25
    attn_level = math.sqrt((1.0 + 0.5 * math.log(SEQ_LEN)) / math.sqrt(SEQ_LEN))
    out_gain = 0.5 / attn_level
    proj_gain = jnp.array([qk_gain, qk_gain, 1.0], jnp.float32).reshape(1, 1, 3, 1, 1)
    vec_shape = (LAYERS, D_MODEL)
    w_qkv = jax.random.normal(keys[4], (LAYERS, D_MODEL, 3, HEADS, HEAD_DIM), jnp.float32) * proj_gain * D_MODEL ** -0.5
    w_out = jax.random.normal(keys[5], (LAYERS, HEADS, HEAD_DIM, D_MODEL), jnp.float32) * (out_gain * D_MODEL ** -0.5)
    w_up = jax.random.normal(keys[7], (LAYERS, D_MODEL, D_FF), jnp.float32) * D_MODEL ** -0.5
    w_down = jax.random.normal(keys[9], (LAYERS, D_FF, D_MODEL), jnp.float32) * (0.8 * D_FF ** -0.5)
    return {
        "x_tokens": tokens.astype(jnp.bfloat16),
        "ln1_gain": 1.0 + 0.2 * jax.random.normal(keys[0], vec_shape, jnp.float32),
        "ln1_bias": 0.2 * jax.random.normal(keys[1], vec_shape, jnp.float32),
        "ln2_gain": 1.0 + 0.2 * jax.random.normal(keys[2], vec_shape, jnp.float32),
        "ln2_bias": 0.2 * jax.random.normal(keys[3], vec_shape, jnp.float32),
        "w_qkv": w_qkv.astype(jnp.bfloat16),
        "w_out": w_out.astype(jnp.bfloat16),
        "b_out": 0.2 * jax.random.normal(keys[6], vec_shape, jnp.float32),
        "w_up": w_up.astype(jnp.bfloat16),
        "b_up": 0.3 * jax.random.normal(keys[8], (LAYERS, D_FF), jnp.float32),
        "w_down": w_down.astype(jnp.bfloat16),
        "b_down": 0.2 * jax.random.normal(keys[10], vec_shape, jnp.float32),
    }


def layer_norm(resid, gain, shift):
    row_mean = jnp.mean(resid, axis=-1, keepdims=True)
    centered = resid - row_mean
    variance = jnp.mean(centered * centered, axis=-1, keepdims=True)
    return (centered * lax.rsqrt(variance + 1e-5) * gain + shift).astype(jnp.bfloat16)


def attention_head(head_parts):
    queries, keys_all, values_all = head_parts
    scores = jnp.einsum("bqe,bke->bqk", queries.astype(jnp.float32), keys_all.astype(jnp.float32)) / math.sqrt(HEAD_DIM)
    positions = jnp.arange(SEQ_LEN)
    causal = positions[:, None] >= positions[None, :]
    scores = jnp.where(causal, scores, -1e30)
    attn_probs = jax.nn.softmax(scores, axis=-1).astype(jnp.bfloat16)
    return jnp.einsum("bqk,bke->bqe", attn_probs.astype(jnp.float32), values_all.astype(jnp.float32)).astype(jnp.bfloat16)


def layer_step(resid, params):
    ln1_gain, ln1_bias, ln2_gain, ln2_bias, w_qkv, w_out, b_out, w_up, b_up, w_down, b_down = params
    normed = layer_norm(resid, ln1_gain, ln1_bias)
    qkv_proj = jnp.dot(normed.reshape(BATCH * SEQ_LEN, D_MODEL), w_qkv.reshape(D_MODEL, 3 * HEADS * HEAD_DIM), preferred_element_type=jnp.float32).astype(jnp.bfloat16)
    qkv_proj = qkv_proj.reshape(BATCH, SEQ_LEN, 3, HEADS, HEAD_DIM)
    heads_first = jnp.transpose(qkv_proj, (2, 3, 0, 1, 4))
    attn_heads = lax.map(attention_head, (heads_first[0], heads_first[1], heads_first[2]))
    attn_out = jnp.einsum("hbse,hed->bsd", attn_heads.astype(jnp.float32), w_out.astype(jnp.float32))
    resid = resid + (attn_out + b_out)
    normed_mlp = layer_norm(resid, ln2_gain, ln2_bias)
    pre_act = jnp.dot(normed_mlp.reshape(BATCH * SEQ_LEN, D_MODEL), w_up, preferred_element_type=jnp.float32) + b_up
    hidden = jax.nn.gelu(pre_act, approximate=True).astype(jnp.bfloat16)
    mlp_out = jnp.dot(hidden, w_down, preferred_element_type=jnp.float32).reshape(BATCH, SEQ_LEN, D_MODEL)
    resid = resid + (mlp_out + b_down)
    return resid, None


def reference(x_tokens, ln1_gain, ln1_bias, ln2_gain, ln2_bias, w_qkv, w_out, b_out, w_up, b_up, w_down, b_down):
    params = (ln1_gain, ln1_bias, ln2_gain, ln2_bias, w_qkv, w_out, b_out, w_up, b_up, w_down, b_down)
    resid, _ = lax.scan(layer_step, x_tokens.astype(jnp.float32), params)
    return resid.astype(jnp.bfloat16)
```

```python
import functools
import math
import jax
import jax.numpy as jnp
from jax import lax
from jax.experimental import pallas as pl
from jax.experimental.pallas import tpu as pltpu
from jax.sharding import PartitionSpec as P

F32 = jnp.float32
BF16 = jnp.bfloat16
LANES = 128
CHUNK = 32
AHEAD = 2
MESH = pl.DeviceIdType.MESH


def layer_norm(resid, gain, shift):
    row_mean = jnp.mean(resid, axis=-1, keepdims=True)
    centered = resid - row_mean
    variance = jnp.mean(centered * centered, axis=-1, keepdims=True)
    return (centered * lax.rsqrt(variance + 1e-5) * gain + shift).astype(BF16)


def col_tiles(width, tile=512):
    return [(start, min(tile, width - start)) for start in range(0, width, tile)]


def chunk_place(j, chips, per_core):
    turn = (j // 2) % chips
    owner = jnp.where(turn % 2 == 0, turn // 2, chips - 1 - turn // 2)
    return owner, (j // (2 * chips)) * 2 + j % 2


def exchange_kernel(chips, per_core, act, final, *refs):
    if final:
        (x_ref, w_ref, resid_ref, bias_ref, out_ref, part, other, inc, inc2, acc_ref,
         part_s, part_r, sum_s, inc_r, inc2_r) = refs
    else:
        (x_ref, w_ref, resid_ref, bias_ref, gain_ref, shift_ref, w2_ref, b2_ref, out_ref, resid_out, part, other, inc, inc2,
         acc_ref, normed, part_s, part_r, sum_s, inc_r, inc2_r, norm_r, left_s, right_s, mate_s, mate_r) = refs
    n_chunks = chips * per_core
    far = chips - 1
    group = lax.axis_index("dp")
    me = lax.axis_index("tp")
    z, core = me // 2, me % 2
    mate = (group, z * 2 + (1 - core))
    left = (group, jnp.maximum(me - 2, 0))
    right = (group, jnp.minimum(me + 2, 2 * chips - 1))
    has_left, has_right = z > 0, z < far

    def remote(src, dst, send, recv, device):
        return pltpu.make_async_remote_copy(src_ref=src, dst_ref=dst, send_sem=send, recv_sem=recv, device_id=device, device_id_type=MESH)

    barrier = pltpu.get_barrier_semaphore()
    pl.semaphore_signal(barrier, inc=1, device_id=mate, device_id_type=MESH)

    @pl.when(has_left)
    def _():
        pl.semaphore_signal(barrier, inc=1, device_id=left, device_id_type=MESH)

    @pl.when(has_right)
    def _():
        pl.semaphore_signal(barrier, inc=1, device_id=right, device_id_type=MESH)

    pl.semaphore_wait(barrier, 1 + has_left.astype(jnp.int32) + has_right.astype(jnp.int32))

    def matmul_in(j):
        owner, place = chunk_place(j, chips, per_core)
        rows = x_ref[owner, :, pl.ds(place, 2)].reshape(4 * CHUNK, x_ref.shape[-1])
        for start, width in col_tiles(w_ref.shape[1]):
            tile = jnp.dot(rows, w_ref[:, start : start + width], preferred_element_type=F32)
            part[owner, :, pl.ds(place, 2), :, start : start + width] = tile.astype(BF16).reshape(2, 2, CHUNK, width)
        for half in range(2):
            remote(part.at[owner, 1 - core, place + half], other.at[owner, place + half], part_s.at[j + half], part_r.at[j + half], mate).start()

    def own_sum(j, owner, place):
        mine = part.at[owner, core, place]
        remote(mine, other.at[owner, place], part_s.at[j], part_r.at[j], mate).wait_recv()
        acc_ref[...] = mine[...].astype(F32) + other[owner, place].astype(F32)

    def add_inc(j, owner, place):
        remote(inc.at[owner, place], inc.at[owner, place], sum_s.at[j], inc_r.at[j], left).wait_recv()
        acc_ref[...] += inc[owner, place].astype(F32)

    def pass_sum(j, owner, place):
        own_sum(j, owner, place)

        @pl.when(jnp.where(z < owner, has_left, has_right))
        def _():
            add_inc(j, owner, place)

        mine = part.at[owner, core, place]
        mine[...] = acc_ref[...].astype(BF16)

        @pl.when(z < owner)
        def _():
            remote(mine, inc.at[owner, place], sum_s.at[j], inc_r.at[j], right).start()

        @pl.when(z > owner + 1)
        def _():
            remote(mine, inc.at[owner, place], sum_s.at[j], inc_r.at[j], left).start()

        @pl.when(z == owner + 1)
        def _():
            remote(mine, inc2.at[place], sum_s.at[j], inc2_r.at[j], left).start()

    def send_left(j, rows):
        remote(rows, rows, left_s.at[j], norm_r.at[j], left).start()

    def send_right(j, rows):
        remote(rows, rows, right_s.at[j], norm_r.at[j], right).start()

    def finish_sum(j, owner, place):
        own_sum(j, owner, place)

        @pl.when(has_left)
        def _():
            add_inc(j, owner, place)

        @pl.when(has_right)
        def _():
            remote(inc2.at[place], inc2.at[place], sum_s.at[j], inc2_r.at[j], right).wait_recv()
            acc_ref[...] += inc2[place].astype(F32)

        resid = resid_ref[place] + (acc_ref[...] + bias_ref[...])
        if final:
            out_ref[place] = resid.astype(BF16)
            return
        resid_out[place] = resid
        rows = normed.at[owner, core, place]
        rows[...] = layer_norm(resid, gain_ref[...], shift_ref[...])
        pl.when(has_left)(lambda: send_left(j, rows))
        pl.when(has_right)(lambda: send_right(j, rows))
        remote(rows, rows, mate_s.at[j], mate_r.at[j], mate).start()

    def pass_norm(j, owner, place):
        rows = normed.at[owner, core, place]
        remote(rows, rows, left_s.at[j], norm_r.at[j], left).wait_recv()
        pl.when((z < owner) & has_left)(lambda: send_left(j, rows))
        pl.when((z > owner) & has_right)(lambda: send_right(j, rows))
        remote(rows, rows, mate_s.at[j], mate_r.at[j], mate).start()

    def matmul_out(j):
        owner, place = chunk_place(j, chips, per_core)
        for half in range(2):
            rows = normed.at[owner, 1 - core, place + half]
            remote(rows, rows, mate_s.at[j + half], mate_r.at[j + half], mate).wait_recv()
        rows = normed[owner, :, pl.ds(place, 2)].reshape(4 * CHUNK, normed.shape[-1])
        for start, width in col_tiles(w2_ref.shape[1]):
            tile = jnp.dot(rows, w2_ref[:, start : start + width], preferred_element_type=F32)
            if act:
                tile = jax.nn.gelu(tile + b2_ref[:, start : start + width], approximate=True)
            out_ref[owner, :, pl.ds(place, 2), :, start : start + width] = tile.astype(BF16).reshape(2, 2, CHUNK, width)

    def at_distance(j, distance, step):
        inside = (j >= 0) & (j < n_chunks)
        safe = jnp.clip(j, 0, n_chunks - 1)
        owner, place = chunk_place(safe, chips, per_core)
        pl.when(inside & (jnp.abs(z - owner) == distance))(lambda: step(safe, owner, place))

    def tick(t, carry):
        for distance in range(far, -1, -1):
            at_distance(t - AHEAD - far + distance, distance, finish_sum if distance == 0 else pass_sum)
        if not final:
            for distance in range(1, chips):
                at_distance(t - AHEAD - far - distance, distance, pass_norm)

        @pl.when((t % 2 == 0) & (t < n_chunks))
        def _():
            matmul_in(jnp.clip(t, 0, n_chunks - 2))

        if not final:
            late = t - AHEAD - 2 * far - 2

            @pl.when((t % 2 == 0) & (late >= 0))
            def _():
                matmul_out(jnp.clip(late, 0, n_chunks - 2))

        return carry

    ticks = n_chunks + AHEAD + far if final else n_chunks + AHEAD + 2 * far + 1
    lax.fori_loop(0, ticks, tick, 0)

    def drain(j, carry):
        owner, place = chunk_place(j, chips, per_core)
        mine = part.at[owner, core, place]
        remote(mine, other.at[owner, place], part_s.at[j], part_r.at[j], mate).wait_send()

        @pl.when(z != owner)
        def _():
            remote(mine, inc.at[owner, place], sum_s.at[j], inc_r.at[j], left).wait_send()

        if not final:
            rows = normed.at[owner, core, place]

            @pl.when((z <= owner) & has_left)
            def _():
                remote(rows, rows, left_s.at[j], norm_r.at[j], left).wait_send()

            @pl.when((z >= owner) & has_right)
            def _():
                remote(rows, rows, right_s.at[j], norm_r.at[j], right).wait_send()

            remote(rows, rows, mate_s.at[j], mate_r.at[j], mate).wait_send()
        return carry

    lax.fori_loop(0, n_chunks, drain, 0)


def exchange(chips, call_id, x, w, resid, bias, norm=None, w2=None, b2=None):
    seq_len, depth = x.shape
    width = w.shape[1]
    own = resid.shape[0]
    per_core = own // CHUNK
    n_chunks = chips * per_core
    final = norm is None
    blocks = (chips, 2, per_core, CHUNK)
    operands = [x.reshape(*blocks, depth), w, resid.reshape(per_core, CHUNK, width), bias[None]]
    scratch = [
        pltpu.VMEM((*blocks, width), BF16),
        pltpu.VMEM((chips, per_core, CHUNK, width), BF16),
        pltpu.VMEM((chips, per_core, CHUNK, width), BF16),
        pltpu.VMEM((per_core, CHUNK, width), BF16),
        pltpu.VMEM((CHUNK, width), F32),
    ]
    sems = [pltpu.SemaphoreType.DMA((n_chunks,))]
    flops = 2 * seq_len * depth * width
    if final:
        out_shape = jax.ShapeDtypeStruct((per_core, CHUNK, width), BF16)
        scratch += sems * 5
    else:
        width2 = w2.shape[1]
        operands += [norm[0][None], norm[1][None], w2, jnp.zeros((1, width2), F32) if b2 is None else b2[None]]
        out_shape = (jax.ShapeDtypeStruct((*blocks, width2), BF16), jax.ShapeDtypeStruct((per_core, CHUNK, width), F32))
        scratch += [pltpu.VMEM((*blocks, width), BF16)] + sems * 10
        flops += 2 * seq_len * width * width2
    vmem = pl.BlockSpec(memory_space=pltpu.VMEM)
    result = pl.pallas_call(
        functools.partial(exchange_kernel, chips, per_core, b2 is not None, final),
        out_shape=out_shape,
        in_specs=[vmem] * len(operands),
        out_specs=vmem if final else (vmem, vmem),
        scratch_shapes=scratch,
        compiler_params=pltpu.CompilerParams(collective_id=call_id, has_side_effects=True, vmem_limit_bytes=67043328),
        cost_estimate=pl.CostEstimate(flops=flops, bytes_accessed=40 << 20, transcendentals=0),
        name=f"exchange{call_id}",
    )(*operands)
    if final:
        return result.reshape(own, width)
    return result[0].reshape(seq_len, width2), result[1].reshape(own, width)


def attention_kernel(scale, block, q_ref, k_ref, v_ref, o_ref):
    seq_len = q_ref.shape[0]
    slope = scale * math.log2(math.e)
    row = lax.broadcasted_iota(jnp.int32, (block, block), 0)
    col = lax.broadcasted_iota(jnp.int32, (block, block), 1)
    contract = (((1,), (1,)), ((), ()))
    for start in range(0, seq_len, block):
        end = start + block
        q = q_ref[start:end]
        diag = lax.dot_general(q, k_ref[start:end], contract, preferred_element_type=F32)
        diag = jnp.where(row >= col, diag, -1e30)
        top = jnp.max(diag, axis=-1, keepdims=True)
        if start:
            past = lax.dot_general(q, k_ref[:start], contract, preferred_element_type=F32)
            top = jnp.maximum(top, jnp.max(past, axis=-1, keepdims=True))
        shift = top * slope
        diag = jnp.exp2(diag * slope - shift)
        total = jnp.sum(diag, axis=-1, keepdims=True)
        if start:
            past = jnp.exp2(past * slope - shift)
            total = total + jnp.sum(past, axis=-1, keepdims=True)
        inv = 1.0 / total
        out = jnp.dot((diag * inv).astype(BF16), v_ref[start:end], preferred_element_type=F32)
        if start:
            out = out + jnp.dot((past * inv).astype(BF16), v_ref[:start], preferred_element_type=F32)
        o_ref[start:end] = out.astype(BF16)


def attention(qkv, heads, scale):
    seq_len = qkv.shape[0]
    spec = lambda first: pl.BlockSpec((seq_len, LANES), lambda h: (0, first + h))
    return pl.pallas_call(
        functools.partial(attention_kernel, scale, 256),
        grid=(heads,),
        out_shape=jax.ShapeDtypeStruct((seq_len, heads * LANES), BF16),
        in_specs=[spec(0), spec(heads), spec(2 * heads)],
        out_specs=spec(0),
        compiler_params=pltpu.CompilerParams(vmem_limit_bytes=50 << 20),
        cost_estimate=pl.CostEstimate(flops=2 * heads * seq_len * seq_len * LANES, bytes_accessed=8 << 20, transcendentals=heads * seq_len * seq_len // 2),
        name="attention",
    )(qkv, qkv, qkv)


def solution(mesh):
    tp_size = mesh.shape["tp"]
    chips = tp_size // 2

    def local_forward(x_local, ln1_gain, ln1_bias, ln2_gain, ln2_bias, w_qkv, w_out, b_out, w_up, b_up, w_down, b_down):
        layers, width, _, heads, head_dim = w_qkv.shape
        scale = 1.0 / math.sqrt(head_dim)
        pad = LANES - head_dim
        wq = jnp.pad(w_qkv, ((0, 0), (0, 0), (0, 0), (0, 0), (0, pad))).reshape(layers, width, 3 * heads * LANES)
        wo = jnp.pad(w_out, ((0, 0), (0, 0), (0, pad), (0, 0))).reshape(layers, heads * LANES, width)
        resid = x_local[0].astype(F32)
        normed = layer_norm(resid, ln1_gain[0], ln1_bias[0])
        gathered = lax.all_gather(normed, "tp", axis=0, tiled=True)
        qkv = jnp.dot(gathered, wq[0], preferred_element_type=F32).astype(BF16)
        call_id = 0
        for layer in range(layers):
            heads_out = attention(qkv, heads, scale)
            hidden, resid = exchange(chips, call_id, heads_out, wo[layer], resid, b_out[layer],
                                     (ln2_gain[layer], ln2_bias[layer]), w_up[layer], b_up[layer])
            if layer + 1 < layers:
                qkv, resid = exchange(chips, call_id + 1, hidden, w_down[layer], resid, b_down[layer],
                                      (ln1_gain[layer + 1], ln1_bias[layer + 1]), wq[layer + 1])
            else:
                out = exchange(chips, call_id + 1, hidden, w_down[layer], resid, b_down[layer])
            call_id += 2
        return out[None]

    rows_spec = P("dp", "tp", None)
    in_specs = (rows_spec, P(), P(), P(), P(), P(None, None, None, "tp", None), P(None, "tp", None, None), P(), P(None, None, "tp"), P(None, "tp"), P(None, "tp", None), P())
    return jax.shard_map(local_forward, mesh=mesh, in_specs=in_specs, out_specs=rows_spec, check_vma=False)
```

```python
import functools
import math
import jax
import jax.numpy as jnp
from jax import lax
from jax.experimental import pallas as pl
from jax.experimental.pallas import tpu as pltpu
from jax.sharding import PartitionSpec as P

F32 = jnp.float32
BF16 = jnp.bfloat16
LANES = 128
CHUNK = 16
AHEAD = 4
HOP = 4
MESH = pl.DeviceIdType.MESH


def layer_norm(resid, gain, shift):
    row_mean = jnp.mean(resid, axis=-1, keepdims=True)
    centered = resid - row_mean
    variance = jnp.mean(centered * centered, axis=-1, keepdims=True)
    return (centered * lax.rsqrt(variance + 1e-5) * gain + shift).astype(BF16)


def col_tiles(width, tile=512):
    return [(start, min(tile, width - start)) for start in range(0, width, tile)]


def owner_of(turn, chips):
    if isinstance(turn, int):
        return turn // 2 if turn % 2 == 0 else chips - 1 - turn // 2
    return jnp.where(turn % 2 == 0, turn // 2, chips - 1 - turn // 2)


def chunk_place(j, chips):
    return owner_of(j % chips, chips), j // chips


def exchange_kernel(chips, per_core, act, final, *refs):
    if final:
        (x_ref, w_ref, resid_ref, bias_ref, out_ref, part, other, inc, inc2, acc_ref,
         part_s, part_r, sum_s, inc_r, inc2_r) = refs
    else:
        (x_ref, w_ref, resid_ref, bias_ref, gain_ref, shift_ref, w2_ref, b2_ref, out_ref, resid_out, part, other, inc, inc2,
         acc_ref, normed, part_s, part_r, sum_s, inc_r, inc2_r, norm_r, left_s, right_s, mate_s, mate_r) = refs
    n_chunks = chips * per_core
    far = chips - 1
    group_rows = chips * 2 * CHUNK
    group = lax.axis_index("dp")
    me = lax.axis_index("tp")
    z, core = me // 2, me % 2
    mate = (group, z * 2 + (1 - core))
    left = (group, jnp.maximum(me - 2, 0))
    right = (group, jnp.minimum(me + 2, 2 * chips - 1))
    has_left, has_right = z > 0, z < far

    def remote(src, dst, send, recv, device):
        return pltpu.make_async_remote_copy(src_ref=src, dst_ref=dst, send_sem=send, recv_sem=recv, device_id=device, device_id_type=MESH)

    barrier = pltpu.get_barrier_semaphore()
    pl.semaphore_signal(barrier, inc=1, device_id=mate, device_id_type=MESH)

    @pl.when(has_left)
    def _():
        pl.semaphore_signal(barrier, inc=1, device_id=left, device_id_type=MESH)

    @pl.when(has_right)
    def _():
        pl.semaphore_signal(barrier, inc=1, device_id=right, device_id_type=MESH)

    pl.semaphore_wait(barrier, 1 + has_left.astype(jnp.int32) + has_right.astype(jnp.int32))

    def matmul_in(j):
        place = j // chips
        rows = x_ref[:, :, place].reshape(group_rows, x_ref.shape[-1])
        for start, width in col_tiles(w_ref.shape[1]):
            tile = jnp.dot(rows, w_ref[:, start : start + width], preferred_element_type=F32)
            part[:, :, place, :, start : start + width] = tile.astype(BF16).reshape(chips, 2, CHUNK, width)
        for turn in range(chips):
            owner = owner_of(turn, chips)
            remote(part.at[owner, 1 - core, place], other.at[owner, place], part_s.at[j + turn], part_r.at[j + turn], mate).start()

    def own_sum(j, owner, place):
        mine = part.at[owner, core, place]
        remote(mine, other.at[owner, place], part_s.at[j], part_r.at[j], mate).wait_recv()
        acc_ref[...] = mine[...].astype(F32) + other[owner, place].astype(F32)

    def add_inc(j, owner, place):
        remote(inc.at[owner, place], inc.at[owner, place], sum_s.at[j], inc_r.at[j], left).wait_recv()
        acc_ref[...] += inc[owner, place].astype(F32)

    def pass_sum(j, owner, place):
        own_sum(j, owner, place)

        @pl.when(jnp.where(z < owner, has_left, has_right))
        def _():
            add_inc(j, owner, place)

        mine = part.at[owner, core, place]
        mine[...] = acc_ref[...].astype(BF16)

        @pl.when(z < owner)
        def _():
            remote(mine, inc.at[owner, place], sum_s.at[j], inc_r.at[j], right).start()

        @pl.when(z > owner + 1)
        def _():
            remote(mine, inc.at[owner, place], sum_s.at[j], inc_r.at[j], left).start()

        @pl.when(z == owner + 1)
        def _():
            remote(mine, inc2.at[place], sum_s.at[j], inc2_r.at[j], left).start()

    def send_left(j, rows):
        remote(rows, rows, left_s.at[j], norm_r.at[j], left).start()

    def send_right(j, rows):
        remote(rows, rows, right_s.at[j], norm_r.at[j], right).start()

    def finish_sum(j, owner, place):
        own_sum(j, owner, place)

        @pl.when(has_left)
        def _():
            add_inc(j, owner, place)

        @pl.when(has_right)
        def _():
            remote(inc2.at[place], inc2.at[place], sum_s.at[j], inc2_r.at[j], right).wait_recv()
            acc_ref[...] += inc2[place].astype(F32)

        resid = resid_ref[place] + (acc_ref[...] + bias_ref[...])
        if final:
            out_ref[place] = resid.astype(BF16)
            return
        resid_out[place] = resid
        rows = normed.at[owner, core, place]
        rows[...] = layer_norm(resid, gain_ref[...], shift_ref[...])
        pl.when(has_left)(lambda: send_left(j, rows))
        pl.when(has_right)(lambda: send_right(j, rows))
        remote(rows, rows, mate_s.at[j], mate_r.at[j], mate).start()

    def pass_norm(j, owner, place):
        rows = normed.at[owner, core, place]
        remote(rows, rows, left_s.at[j], norm_r.at[j], left).wait_recv()
        pl.when((z < owner) & has_left)(lambda: send_left(j, rows))
        pl.when((z > owner) & has_right)(lambda: send_right(j, rows))
        remote(rows, rows, mate_s.at[j], mate_r.at[j], mate).start()

    def matmul_out(j):
        place = j // chips
        for turn in range(chips):
            rows = normed.at[owner_of(turn, chips), 1 - core, place]
            remote(rows, rows, mate_s.at[j + turn], mate_r.at[j + turn], mate).wait_recv()
        rows = normed[:, :, place].reshape(group_rows, normed.shape[-1])
        for start, width in col_tiles(w2_ref.shape[1]):
            tile = jnp.dot(rows, w2_ref[:, start : start + width], preferred_element_type=F32)
            if act:
                tile = jax.nn.gelu(tile + b2_ref[:, start : start + width], approximate=True)
            out_ref[:, :, place, :, start : start + width] = tile.astype(BF16).reshape(chips, 2, CHUNK, width)

    def at_distance(j, distance, step):
        inside = (j >= 0) & (j < n_chunks)
        safe = jnp.clip(j, 0, n_chunks - 1)
        owner, place = chunk_place(safe, chips)
        pl.when(inside & (jnp.abs(z - owner) == distance))(lambda: step(safe, owner, place))

    def tick(t, carry):
        for distance in range(far, -1, -1):
            at_distance(t - AHEAD - HOP * (far - distance), distance, finish_sum if distance == 0 else pass_sum)
        if not final:
            for distance in range(1, chips):
                at_distance(t - AHEAD - HOP * (far + distance), distance, pass_norm)

        @pl.when((t % chips == 0) & (t < n_chunks))
        def _():
            matmul_in(jnp.clip(t, 0, n_chunks - chips))

        if not final:
            late = t - AHEAD - 2 * HOP * far - chips

            @pl.when((late % chips == 0) & (late >= 0))
            def _():
                matmul_out(jnp.clip(late, 0, n_chunks - chips))

        return carry

    ticks = n_chunks + AHEAD + HOP * far if final else n_chunks + AHEAD + 2 * HOP * far + 1
    lax.fori_loop(0, ticks, tick, 0)

    def drain(j, carry):
        owner, place = chunk_place(j, chips)
        mine = part.at[owner, core, place]
        remote(mine, other.at[owner, place], part_s.at[j], part_r.at[j], mate).wait_send()

        @pl.when(z != owner)
        def _():
            remote(mine, inc.at[owner, place], sum_s.at[j], inc_r.at[j], left).wait_send()

        if not final:
            rows = normed.at[owner, core, place]

            @pl.when((z <= owner) & has_left)
            def _():
                remote(rows, rows, left_s.at[j], norm_r.at[j], left).wait_send()

            @pl.when((z >= owner) & has_right)
            def _():
                remote(rows, rows, right_s.at[j], norm_r.at[j], right).wait_send()

            remote(rows, rows, mate_s.at[j], mate_r.at[j], mate).wait_send()
        return carry

    lax.fori_loop(0, n_chunks, drain, 0)


def exchange(chips, call_id, x, w, resid, bias, norm=None, w2=None, b2=None):
    seq_len, depth = x.shape
    width = w.shape[1]
    own = resid.shape[0]
    per_core = own // CHUNK
    n_chunks = chips * per_core
    final = norm is None
    blocks = (chips, 2, per_core, CHUNK)
    operands = [x.reshape(*blocks, depth), w, resid.reshape(per_core, CHUNK, width), bias[None]]
    scratch = [
        pltpu.VMEM((*blocks, width), BF16),
        pltpu.VMEM((chips, per_core, CHUNK, width), BF16),
        pltpu.VMEM((chips, per_core, CHUNK, width), BF16),
        pltpu.VMEM((per_core, CHUNK, width), BF16),
        pltpu.VMEM((CHUNK, width), F32),
    ]
    sems = [pltpu.SemaphoreType.DMA((n_chunks,))]
    flops = 2 * seq_len * depth * width
    if final:
        out_shape = jax.ShapeDtypeStruct((per_core, CHUNK, width), BF16)
        scratch += sems * 5
    else:
        width2 = w2.shape[1]
        operands += [norm[0][None], norm[1][None], w2, jnp.zeros((1, width2), F32) if b2 is None else b2[None]]
        out_shape = (jax.ShapeDtypeStruct((*blocks, width2), BF16), jax.ShapeDtypeStruct((per_core, CHUNK, width), F32))
        scratch += [pltpu.VMEM((*blocks, width), BF16)] + sems * 10
        flops += 2 * seq_len * width * width2
    vmem = pl.BlockSpec(memory_space=pltpu.VMEM)
    result = pl.pallas_call(
        functools.partial(exchange_kernel, chips, per_core, b2 is not None, final),
        out_shape=out_shape,
        in_specs=[vmem] * len(operands),
        out_specs=vmem if final else (vmem, vmem),
        scratch_shapes=scratch,
        compiler_params=pltpu.CompilerParams(collective_id=call_id, has_side_effects=True, vmem_limit_bytes=67043328),
        cost_estimate=pl.CostEstimate(flops=flops, bytes_accessed=40 << 20, transcendentals=0),
        name=f"exchange{call_id}",
    )(*operands)
    if final:
        return result.reshape(own, width)
    return result[0].reshape(seq_len, width2), result[1].reshape(own, width)


def attention_kernel(scale, block, q_ref, k_ref, v_ref, o_ref):
    seq_len = q_ref.shape[0]
    slope = scale * math.log2(math.e)
    row = lax.broadcasted_iota(jnp.int32, (block, block), 0)
    col = lax.broadcasted_iota(jnp.int32, (block, block), 1)
    contract = (((1,), (1,)), ((), ()))
    for start in range(0, seq_len, block):
        end = start + block
        q = q_ref[start:end]
        diag = lax.dot_general(q, k_ref[start:end], contract, preferred_element_type=F32)
        diag = jnp.where(row >= col, diag, -1e30)
        top = jnp.max(diag, axis=-1, keepdims=True)
        if start:
            past = lax.dot_general(q, k_ref[:start], contract, preferred_element_type=F32)
            top = jnp.maximum(top, jnp.max(past, axis=-1, keepdims=True))
        shift = top * slope
        diag = jnp.exp2(diag * slope - shift)
        total = jnp.sum(diag, axis=-1, keepdims=True)
        if start:
            past = jnp.exp2(past * slope - shift)
            total = total + jnp.sum(past, axis=-1, keepdims=True)
        inv = 1.0 / total
        out = jnp.dot((diag * inv).astype(BF16), v_ref[start:end], preferred_element_type=F32)
        if start:
            out = out + jnp.dot((past * inv).astype(BF16), v_ref[:start], preferred_element_type=F32)
        o_ref[start:end] = out.astype(BF16)


def attention(qkv, heads, scale):
    seq_len = qkv.shape[0]
    spec = lambda first: pl.BlockSpec((seq_len, LANES), lambda h: (0, first + h))
    return pl.pallas_call(
        functools.partial(attention_kernel, scale, 256),
        grid=(heads,),
        out_shape=jax.ShapeDtypeStruct((seq_len, heads * LANES), BF16),
        in_specs=[spec(0), spec(heads), spec(2 * heads)],
        out_specs=spec(0),
        compiler_params=pltpu.CompilerParams(vmem_limit_bytes=50 << 20),
        cost_estimate=pl.CostEstimate(flops=2 * heads * seq_len * seq_len * LANES, bytes_accessed=8 << 20, transcendentals=heads * seq_len * seq_len // 2),
        name="attention",
    )(qkv, qkv, qkv)


def solution(mesh):
    tp_size = mesh.shape["tp"]
    chips = tp_size // 2

    def local_forward(x_local, ln1_gain, ln1_bias, ln2_gain, ln2_bias, w_qkv, w_out, b_out, w_up, b_up, w_down, b_down):
        layers, width, _, heads, head_dim = w_qkv.shape
        scale = 1.0 / math.sqrt(head_dim)
        pad = LANES - head_dim
        wq = jnp.pad(w_qkv, ((0, 0), (0, 0), (0, 0), (0, 0), (0, pad))).reshape(layers, width, 3 * heads * LANES)
        wo = jnp.pad(w_out, ((0, 0), (0, 0), (0, pad), (0, 0))).reshape(layers, heads * LANES, width)
        resid = x_local[0].astype(F32)
        normed = layer_norm(resid, ln1_gain[0], ln1_bias[0])
        gathered = lax.all_gather(normed, "tp", axis=0, tiled=True)
        qkv = jnp.dot(gathered, wq[0], preferred_element_type=F32).astype(BF16)
        call_id = 0
        for layer in range(layers):
            heads_out = attention(qkv, heads, scale)
            hidden, resid = exchange(chips, call_id, heads_out, wo[layer], resid, b_out[layer],
                                     (ln2_gain[layer], ln2_bias[layer]), w_up[layer], b_up[layer])
            if layer + 1 < layers:
                qkv, resid = exchange(chips, call_id + 1, hidden, w_down[layer], resid, b_down[layer],
                                      (ln1_gain[layer + 1], ln1_bias[layer + 1]), wq[layer + 1])
            else:
                out = exchange(chips, call_id + 1, hidden, w_down[layer], resid, b_down[layer])
            call_id += 2
        return out[None]

    rows_spec = P("dp", "tp", None)
    in_specs = (rows_spec, P(), P(), P(), P(), P(None, None, None, "tp", None), P(None, "tp", None, None), P(), P(None, None, "tp"), P(None, "tp"), P(None, "tp", None), P())
    return jax.shard_map(local_forward, mesh=mesh, in_specs=in_specs, out_specs=rows_spec, check_vma=False)
```

```python
import functools
import math
import jax
import jax.numpy as jnp
from jax import lax
from jax.experimental import pallas as pl
from jax.experimental.pallas import tpu as pltpu
from jax.sharding import PartitionSpec as P

F32 = jnp.float32
BF16 = jnp.bfloat16
LANES = 128
CHUNK = 16
AHEAD = 4
HOP = 4
MESH = pl.DeviceIdType.MESH


def layer_norm(resid, gain, shift):
    row_mean = jnp.mean(resid, axis=-1, keepdims=True)
    centered = resid - row_mean
    variance = jnp.mean(centered * centered, axis=-1, keepdims=True)
    return (centered * lax.rsqrt(variance + 1e-5) * gain + shift).astype(BF16)


def col_tiles(width, tile=512):
    return [(start, min(tile, width - start)) for start in range(0, width, tile)]


def owner_of(turn, chips):
    if isinstance(turn, int):
        return turn // 2 if turn % 2 == 0 else chips - 1 - turn // 2
    return jnp.where(turn % 2 == 0, turn // 2, chips - 1 - turn // 2)


def chunk_place(j, chips):
    return owner_of(j % chips, chips), j // chips


class Stage:
    def __init__(self, start, bufs, sems, bias, gain=None, shift=None):
        self.start, self.bias, self.gain, self.shift = start, bias, gain, shift
        self.final = gain is None
        self.part, self.other, self.inc, self.inc2 = bufs[:4]
        self.part_s, self.part_r, self.sum_s, self.inc_r, self.inc2_r = sems[:5]
        if not self.final:
            self.normed = bufs[4]
            self.norm_r, self.left_s, self.right_s, self.mate_s, self.mate_r = sems[5:]


def layer_kernel(chips, per_core, span, layer, final, *refs):
    refs = list(refs)
    take = lambda n: [refs.pop(0) for _ in range(n)]
    x_hbm, resid_hbm, w_out_hbm, w_up_hbm, w_down_hbm, bias_a, gain_a, shift_a, b_up, bias_b = take(10)
    if final:
        (y_ref,) = take(1)
    else:
        w_qkv_hbm, gain_b, shift_b, qkv_hbm, resid = take(5)
    x_ref, w_out, w_up, w_down, hidden, acc_ref, copy_s = take(7)
    stage_a = Stage(0, take(5), take(10), bias_a, gain_a, shift_a)
    if final:
        stage_b = Stage(span, take(4), take(5), bias_b)
        (resid,) = take(1)
    else:
        stage_b = Stage(span, take(5), take(10), bias_b, gain_b, shift_b)
        w_qkv, qkv_buf, qkv_s = take(3)
    n_chunks = chips * per_core
    far = chips - 1
    ring = span // chips
    group_rows = chips * 2 * CHUNK
    group = lax.axis_index("dp")
    me = lax.axis_index("tp")
    z, core = me // 2, me % 2
    mate = (group, z * 2 + (1 - core))
    left = (group, jnp.maximum(me - 2, 0))
    right = (group, jnp.minimum(me + 2, 2 * chips - 1))
    has_left, has_right = z > 0, z < far

    loads = [(x_hbm, x_ref), (w_out_hbm, w_out), (resid_hbm, resid), (w_up_hbm.at[layer], w_up), (w_down_hbm.at[layer], w_down)]
    if not final:
        loads.append((w_qkv_hbm, w_qkv))
    loads = [pltpu.make_async_copy(src, dst, copy_s.at[i]) for i, (src, dst) in enumerate(loads)]
    for load in loads:
        load.start()

    def remote(src, dst, send, recv, device):
        return pltpu.make_async_remote_copy(src_ref=src, dst_ref=dst, send_sem=send, recv_sem=recv, device_id=device, device_id_type=MESH)

    barrier = pltpu.get_barrier_semaphore()
    pl.semaphore_signal(barrier, inc=1, device_id=mate, device_id_type=MESH)

    @pl.when(has_left)
    def _():
        pl.semaphore_signal(barrier, inc=1, device_id=left, device_id_type=MESH)

    @pl.when(has_right)
    def _():
        pl.semaphore_signal(barrier, inc=1, device_id=right, device_id_type=MESH)

    pl.semaphore_wait(barrier, 1 + has_left.astype(jnp.int32) + has_right.astype(jnp.int32))
    for load in loads[:3]:
        load.wait()

    def store_part(s, j, rows, w_ref):
        at = (j // chips) % ring
        for start, width in col_tiles(w_ref.shape[1]):
            tile = jnp.dot(rows, w_ref[:, start : start + width], preferred_element_type=F32)
            s.part[:, :, at, :, start : start + width] = tile.astype(BF16).reshape(chips, 2, CHUNK, width)
        for turn in range(chips):
            owner, n = owner_of(turn, chips), (j + turn) % span
            remote(s.part.at[owner, 1 - core, at], s.other.at[owner, at], s.part_s.at[n], s.part_r.at[n], mate).start()

    def own_sum(s, n, owner, at):
        mine = s.part.at[owner, core, at]
        remote(mine, s.other.at[owner, at], s.part_s.at[n], s.part_r.at[n], mate).wait_recv()
        acc_ref[...] = mine[...].astype(F32) + s.other[owner, at].astype(F32)

    def add_inc(s, n, owner, at):
        remote(s.inc.at[owner, at], s.inc.at[owner, at], s.sum_s.at[n], s.inc_r.at[n], left).wait_recv()
        acc_ref[...] += s.inc[owner, at].astype(F32)

    def pass_sum(s, n, owner, place):
        at = place % ring
        own_sum(s, n, owner, at)

        @pl.when(jnp.where(z < owner, has_left, has_right))
        def _():
            add_inc(s, n, owner, at)

        mine = s.part.at[owner, core, at]
        mine[...] = acc_ref[...].astype(BF16)

        @pl.when(z < owner)
        def _():
            remote(mine, s.inc.at[owner, at], s.sum_s.at[n], s.inc_r.at[n], right).start()

        @pl.when(z > owner + 1)
        def _():
            remote(mine, s.inc.at[owner, at], s.sum_s.at[n], s.inc_r.at[n], left).start()

        @pl.when(z == owner + 1)
        def _():
            remote(mine, s.inc2.at[at], s.sum_s.at[n], s.inc2_r.at[n], left).start()

    def send_left(s, n, rows):
        remote(rows, rows, s.left_s.at[n], s.norm_r.at[n], left).start()

    def send_right(s, n, rows):
        remote(rows, rows, s.right_s.at[n], s.norm_r.at[n], right).start()

    def finish_sum(s, n, owner, place):
        at = place % ring
        own_sum(s, n, owner, at)

        @pl.when(has_left)
        def _():
            add_inc(s, n, owner, at)

        @pl.when(has_right)
        def _():
            remote(s.inc2.at[at], s.inc2.at[at], s.sum_s.at[n], s.inc2_r.at[n], right).wait_recv()
            acc_ref[...] += s.inc2[at].astype(F32)

        total = resid[place] + (acc_ref[...] + s.bias[...])
        if s.final:
            y_ref[place] = total.astype(BF16)
            return
        resid[place] = total
        rows = s.normed.at[owner, core, at]
        rows[...] = layer_norm(total, s.gain[...], s.shift[...])
        pl.when(has_left)(lambda: send_left(s, n, rows))
        pl.when(has_right)(lambda: send_right(s, n, rows))
        remote(rows, rows, s.mate_s.at[n], s.mate_r.at[n], mate).start()

    def pass_norm(s, n, owner, place):
        rows = s.normed.at[owner, core, place % ring]
        remote(rows, rows, s.left_s.at[n], s.norm_r.at[n], left).wait_recv()
        pl.when((z < owner) & has_left)(lambda: send_left(s, n, rows))
        pl.when((z > owner) & has_right)(lambda: send_right(s, n, rows))
        remote(rows, rows, s.mate_s.at[n], s.mate_r.at[n], mate).start()

    def normed_rows(s, j):
        at = (j // chips) % ring
        for turn in range(chips):
            rows, n = s.normed.at[owner_of(turn, chips), 1 - core, at], (j + turn) % span
            remote(rows, rows, s.mate_s.at[n], s.mate_r.at[n], mate).wait_recv()
        return s.normed[:, :, at].reshape(group_rows, s.normed.shape[-1])

    def release(s, j):
        at = (j // chips) % ring
        for turn in range(chips):
            owner, n = owner_of(turn, chips), (j + turn) % span
            mine = s.part.at[owner, core, at]
            remote(mine, s.other.at[owner, at], s.part_s.at[n], s.part_r.at[n], mate).wait_send()
            pl.when(z != owner)(remote(mine, s.inc.at[owner, at], s.sum_s.at[n], s.inc_r.at[n], left).wait_send)
            if not s.final:
                rows = s.normed.at[owner, core, at]
                pl.when((z <= owner) & has_left)(remote(rows, rows, s.left_s.at[n], s.norm_r.at[n], left).wait_send)
                pl.when((z >= owner) & has_right)(remote(rows, rows, s.right_s.at[n], s.norm_r.at[n], right).wait_send)
                remote(rows, rows, s.mate_s.at[n], s.mate_r.at[n], mate).wait_send()

    def project_out(j):
        pl.when(j >= span)(lambda: release(stage_a, j - span))
        store_part(stage_a, j, x_ref[:, :, j // chips].reshape(group_rows, x_ref.shape[-1]), w_out)

    def mlp(j):
        @pl.when(j == 0)
        def _():
            loads[3].wait()
            loads[4].wait()

        rows = normed_rows(stage_a, j)
        for start, width in col_tiles(w_up.shape[1]):
            tile = jnp.dot(rows, w_up[:, start : start + width], preferred_element_type=F32)
            hidden[:, start : start + width] = jax.nn.gelu(tile + b_up[:, start : start + width], approximate=True).astype(BF16)
        pl.when(j >= span)(lambda: release(stage_b, j - span))
        store_part(stage_b, j, hidden[...], w_down)

    def qkv_copy(place):
        return pltpu.make_async_copy(qkv_buf.at[place % 2], qkv_hbm.at[:, :, place], qkv_s.at[place % 2])

    def project_qkv(j):
        place = j // chips
        pl.when(j == 0)(lambda: loads[5].wait())
        pl.when(place >= 2)(lambda: qkv_copy(place - 2).wait())
        rows = normed_rows(stage_b, j)
        for start, width in col_tiles(w_qkv.shape[1]):
            tile = jnp.dot(rows, w_qkv[:, start : start + width], preferred_element_type=F32)
            qkv_buf[place % 2, :, :, :, start : start + width] = tile.astype(BF16).reshape(chips, 2, CHUNK, width)
        qkv_copy(place).start()

    def at_distance(s, j, distance, step):
        inside = (j >= 0) & (j < n_chunks)
        safe = jnp.clip(j, 0, n_chunks - 1)
        owner, place = chunk_place(safe, chips)
        pl.when(inside & (jnp.abs(z - owner) == distance))(lambda: step(s, safe % span, owner, place))

    def at_group(j, step):
        pl.when((j >= 0) & (j < n_chunks) & (j % chips == 0))(lambda: step(jnp.clip(j, 0, n_chunks - chips)))

    def tick(t, carry):
        for s in (stage_b, stage_a):
            for distance in range(far, -1, -1):
                at_distance(s, t - s.start - AHEAD - HOP * (far - distance), distance, finish_sum if distance == 0 else pass_sum)
            if not s.final:
                for distance in range(1, chips):
                    at_distance(s, t - s.start - AHEAD - HOP * (far + distance), distance, pass_norm)
        if not final:
            at_group(t - 2 * span, project_qkv)
        at_group(t - span, mlp)
        at_group(t, project_out)
        return carry

    ticks = span + n_chunks + AHEAD + HOP * far if final else 2 * span + n_chunks - chips + 1
    lax.fori_loop(0, ticks, tick, 0)

    def drain(i, carry):
        release(stage_a, n_chunks - span + i * chips)
        release(stage_b, n_chunks - span + i * chips)
        return carry

    lax.fori_loop(0, ring, drain, 0)
    if not final:
        qkv_copy(per_core - 2).wait()
        qkv_copy(per_core - 1).wait()


def layer_tail(chips, layer, x, resid, w_out, w_up, w_down, bias_a, norm_a, b_up, bias_b, norm_b=None, w_qkv=None):
    seq_len, depth = x.shape
    own, width = resid.shape
    mid = w_up.shape[2]
    per_core = own // CHUNK
    final = norm_b is None
    span = AHEAD + 2 * HOP * (chips - 1) + chips
    ring = span // chips
    assert span % chips == 0 and per_core >= ring
    blocks = (chips, 2, per_core, CHUNK)
    any_spec = pl.BlockSpec(memory_space=pl.ANY)
    vmem = pl.BlockSpec(memory_space=pltpu.VMEM)
    operands = [x.reshape(*blocks, depth), resid.reshape(per_core, CHUNK, width), w_out, w_up, w_down,
                bias_a[None], norm_a[0][None], norm_a[1][None], b_up[None], bias_b[None]]
    in_specs = [any_spec] * 5 + [vmem] * 5
    sems = [pltpu.SemaphoreType.DMA((span,))]
    slots = [
        pltpu.VMEM((chips, 2, ring, CHUNK, width), BF16),
        pltpu.VMEM((chips, ring, CHUNK, width), BF16),
        pltpu.VMEM((chips, ring, CHUNK, width), BF16),
        pltpu.VMEM((ring, CHUNK, width), BF16),
    ]
    norm_slots = [pltpu.VMEM((chips, 2, ring, CHUNK, width), BF16)]
    scratch = [
        pltpu.VMEM((*blocks, depth), BF16),
        pltpu.VMEM((depth, width), BF16),
        pltpu.VMEM((width, mid), BF16),
        pltpu.VMEM((mid, width), BF16),
        pltpu.VMEM((chips * 2 * CHUNK, mid), BF16),
        pltpu.VMEM((CHUNK, width), F32),
        pltpu.SemaphoreType.DMA((6,)),
    ] + slots + norm_slots + sems * 10
    flops = 2 * seq_len * width * (depth + 2 * mid)
    if final:
        out_shape = jax.ShapeDtypeStruct((per_core, CHUNK, width), BF16)
        out_specs = vmem
        scratch += slots + sems * 5 + [pltpu.VMEM((per_core, CHUNK, width), F32)]
    else:
        width2 = w_qkv.shape[1]
        operands += [w_qkv, norm_b[0][None], norm_b[1][None]]
        in_specs += [any_spec, vmem, vmem]
        out_shape = (jax.ShapeDtypeStruct((*blocks, width2), BF16), jax.ShapeDtypeStruct((per_core, CHUNK, width), F32))
        out_specs = (any_spec, vmem)
        scratch += slots + norm_slots + sems * 10
        scratch += [pltpu.VMEM((width, width2), BF16), pltpu.VMEM((2, chips, 2, CHUNK, width2), BF16), pltpu.SemaphoreType.DMA((2,))]
        flops += 2 * seq_len * width * width2
    result = pl.pallas_call(
        functools.partial(layer_kernel, chips, per_core, span, layer, final),
        out_shape=out_shape,
        in_specs=in_specs,
        out_specs=out_specs,
        scratch_shapes=scratch,
        compiler_params=pltpu.CompilerParams(collective_id=layer, has_side_effects=True, vmem_limit_bytes=67043328),
        cost_estimate=pl.CostEstimate(flops=flops, bytes_accessed=40 << 20, transcendentals=0),
        name=f"layer{layer}",
    )(*operands)
    if final:
        return result.reshape(own, width)
    return result[0].reshape(seq_len, width2), result[1].reshape(own, width)


def attention_kernel(scale, block, q_ref, k_ref, v_ref, o_ref):
    seq_len = q_ref.shape[0]
    slope = scale * math.log2(math.e)
    row = lax.broadcasted_iota(jnp.int32, (block, block), 0)
    col = lax.broadcasted_iota(jnp.int32, (block, block), 1)
    contract = (((1,), (1,)), ((), ()))
    for start in range(0, seq_len, block):
        end = start + block
        q = q_ref[start:end]
        diag = lax.dot_general(q, k_ref[start:end], contract, preferred_element_type=F32)
        diag = jnp.where(row >= col, diag, -1e30)
        top = jnp.max(diag, axis=-1, keepdims=True)
        if start:
            past = lax.dot_general(q, k_ref[:start], contract, preferred_element_type=F32)
            top = jnp.maximum(top, jnp.max(past, axis=-1, keepdims=True))
        shift = top * slope
        diag = jnp.exp2(diag * slope - shift)
        total = jnp.sum(diag, axis=-1, keepdims=True)
        if start:
            past = jnp.exp2(past * slope - shift)
            total = total + jnp.sum(past, axis=-1, keepdims=True)
        inv = 1.0 / total
        out = jnp.dot((diag * inv).astype(BF16), v_ref[start:end], preferred_element_type=F32)
        if start:
            out = out + jnp.dot((past * inv).astype(BF16), v_ref[:start], preferred_element_type=F32)
        o_ref[start:end] = out.astype(BF16)


def attention(qkv, heads, scale):
    seq_len = qkv.shape[0]
    spec = lambda first: pl.BlockSpec((seq_len, LANES), lambda h: (0, first + h))
    return pl.pallas_call(
        functools.partial(attention_kernel, scale, 256),
        grid=(heads,),
        out_shape=jax.ShapeDtypeStruct((seq_len, heads * LANES), BF16),
        in_specs=[spec(0), spec(heads), spec(2 * heads)],
        out_specs=spec(0),
        compiler_params=pltpu.CompilerParams(vmem_limit_bytes=50 << 20),
        cost_estimate=pl.CostEstimate(flops=2 * heads * seq_len * seq_len * LANES, bytes_accessed=8 << 20, transcendentals=heads * seq_len * seq_len // 2),
        name="attention",
    )(qkv, qkv, qkv)


def solution(mesh):
    tp_size = mesh.shape["tp"]
    chips = tp_size // 2

    def local_forward(x_local, ln1_gain, ln1_bias, ln2_gain, ln2_bias, w_qkv, w_out, b_out, w_up, b_up, w_down, b_down):
        layers, width, _, heads, head_dim = w_qkv.shape
        scale = 1.0 / math.sqrt(head_dim)
        pad = LANES - head_dim
        wq = jnp.pad(w_qkv, ((0, 0), (0, 0), (0, 0), (0, 0), (0, pad))).reshape(layers, width, 3 * heads * LANES)
        wo = jnp.pad(w_out, ((0, 0), (0, 0), (0, pad), (0, 0))).reshape(layers, heads * LANES, width)
        resid = x_local[0].astype(F32)
        normed = layer_norm(resid, ln1_gain[0], ln1_bias[0])
        gathered = lax.all_gather(normed, "tp", axis=0, tiled=True)
        qkv = jnp.dot(gathered, wq[0], preferred_element_type=F32).astype(BF16)
        for layer in range(layers):
            heads_out = attention(qkv, heads, scale)
            args = (chips, layer, heads_out, resid, wo[layer], w_up, w_down, b_out[layer],
                    (ln2_gain[layer], ln2_bias[layer]), b_up[layer], b_down[layer])
            if layer + 1 < layers:
                qkv, resid = layer_tail(*args, (ln1_gain[layer + 1], ln1_bias[layer + 1]), wq[layer + 1])
            else:
                out = layer_tail(*args)
        return out[None]

    rows_spec = P("dp", "tp", None)
    in_specs = (rows_spec, P(), P(), P(), P(), P(None, None, None, "tp", None), P(None, "tp", None, None), P(), P(None, None, "tp"), P(None, "tp"), P(None, "tp", None), P())
    return jax.shard_map(local_forward, mesh=mesh, in_specs=in_specs, out_specs=rows_spec, check_vma=False)
```

```python
import functools
import math
import jax
import jax.numpy as jnp
from jax import lax
from jax.experimental import pallas as pl
from jax.experimental.pallas import tpu as pltpu
from jax.sharding import PartitionSpec as P

F32 = jnp.float32
BF16 = jnp.bfloat16
LANES = 128
CHUNK = 16
AHEAD = 4
HOP = 4
MESH = pl.DeviceIdType.MESH


def layer_norm(resid, gain, shift):
    row_mean = jnp.mean(resid, axis=-1, keepdims=True)
    centered = resid - row_mean
    variance = jnp.mean(centered * centered, axis=-1, keepdims=True)
    return (centered * lax.rsqrt(variance + 1e-5) * gain + shift).astype(BF16)


def col_tiles(width, tile=512):
    return [(start, min(tile, width - start)) for start in range(0, width, tile)]


def owner_of(turn, chips):
    if isinstance(turn, int):
        return turn // 2 if turn % 2 == 0 else chips - 1 - turn // 2
    return jnp.where(turn % 2 == 0, turn // 2, chips - 1 - turn // 2)


def chunk_place(j, chips):
    return owner_of(j % chips, chips), j // chips


class Stage:
    def __init__(self, start, bufs, sems, bias, gain=None, shift=None):
        self.start, self.bias, self.gain, self.shift = start, bias, gain, shift
        self.final = gain is None
        self.part, self.other, self.inc, self.inc2 = bufs[:4]
        self.part_s, self.part_r, self.sum_s, self.inc_r, self.inc2_r = sems[:5]
        if not self.final:
            self.normed = bufs[4]
            self.norm_r, self.left_s, self.right_s, self.mate_s, self.mate_r = sems[5:]


def layer_kernel(chips, per_core, span, layer, final, *refs):
    refs = list(refs)
    take = lambda n: [refs.pop(0) for _ in range(n)]
    x_hbm, resid_hbm, w_out_hbm, w_up_hbm, w_down_hbm, bias_a, gain_a, shift_a, b_up, bias_b = take(10)
    if final:
        (y_ref,) = take(1)
    else:
        w_qkv_hbm, gain_b, shift_b, qkv_hbm, resid = take(5)
    x_ref, w_out, w_up, w_down, hidden, acc_ref, copy_s = take(7)
    stage_a = Stage(0, take(5), take(10), bias_a, gain_a, shift_a)
    if final:
        stage_b = Stage(span, take(4), take(5), bias_b)
        (resid,) = take(1)
    else:
        stage_b = Stage(span, take(5), take(10), bias_b, gain_b, shift_b)
        w_qkv, qkv_buf, qkv_s = take(3)
    n_chunks = chips * per_core
    far = chips - 1
    ring = span // chips
    group_rows = chips * 2 * CHUNK
    group = lax.axis_index("dp")
    me = lax.axis_index("tp")
    z, core = me // 2, me % 2
    mate = (group, z * 2 + (1 - core))
    left = (group, jnp.maximum(me - 2, 0))
    right = (group, jnp.minimum(me + 2, 2 * chips - 1))
    has_left, has_right = z > 0, z < far

    loads = [(x_hbm, x_ref), (w_out_hbm, w_out), (resid_hbm, resid), (w_up_hbm.at[layer], w_up), (w_down_hbm.at[layer], w_down)]
    if not final:
        loads.append((w_qkv_hbm, w_qkv))
    loads = [pltpu.make_async_copy(src, dst, copy_s.at[i]) for i, (src, dst) in enumerate(loads)]
    for load in loads:
        load.start()

    def remote(src, dst, send, recv, device):
        return pltpu.make_async_remote_copy(src_ref=src, dst_ref=dst, send_sem=send, recv_sem=recv, device_id=device, device_id_type=MESH)

    barrier = pltpu.get_barrier_semaphore()
    pl.semaphore_signal(barrier, inc=1, device_id=mate, device_id_type=MESH)

    @pl.when(has_left)
    def _():
        pl.semaphore_signal(barrier, inc=1, device_id=left, device_id_type=MESH)

    @pl.when(has_right)
    def _():
        pl.semaphore_signal(barrier, inc=1, device_id=right, device_id_type=MESH)

    pl.semaphore_wait(barrier, 1 + has_left.astype(jnp.int32) + has_right.astype(jnp.int32))
    for load in loads[:3]:
        load.wait()

    def store_part(s, j, rows, w_ref):
        at = (j // chips) % ring
        for start, width in col_tiles(w_ref.shape[1]):
            tile = jnp.dot(rows, w_ref[:, start : start + width], preferred_element_type=F32)
            s.part[:, :, at, :, start : start + width] = tile.astype(BF16).reshape(chips, 2, CHUNK, width)
        for turn in range(chips):
            owner, n = owner_of(turn, chips), (j + turn) % span
            remote(s.part.at[owner, 1 - core, at], s.other.at[owner, at], s.part_s.at[n], s.part_r.at[n], mate).start()

    def own_sum(s, n, owner, at):
        mine = s.part.at[owner, core, at]
        remote(mine, s.other.at[owner, at], s.part_s.at[n], s.part_r.at[n], mate).wait_recv()
        acc_ref[...] = mine[...].astype(F32) + s.other[owner, at].astype(F32)

    def add_inc(s, n, owner, at):
        remote(s.inc.at[owner, at], s.inc.at[owner, at], s.sum_s.at[n], s.inc_r.at[n], left).wait_recv()
        acc_ref[...] += s.inc[owner, at].astype(F32)

    def pass_sum(s, n, owner, place):
        at = place % ring
        own_sum(s, n, owner, at)

        @pl.when(jnp.where(z < owner, has_left, has_right))
        def _():
            add_inc(s, n, owner, at)

        mine = s.part.at[owner, core, at]
        mine[...] = acc_ref[...].astype(BF16)

        @pl.when(z < owner)
        def _():
            remote(mine, s.inc.at[owner, at], s.sum_s.at[n], s.inc_r.at[n], right).start()

        @pl.when(z > owner + 1)
        def _():
            remote(mine, s.inc.at[owner, at], s.sum_s.at[n], s.inc_r.at[n], left).start()

        @pl.when(z == owner + 1)
        def _():
            remote(mine, s.inc2.at[at], s.sum_s.at[n], s.inc2_r.at[n], left).start()

    def send_left(s, n, rows):
        remote(rows, rows, s.left_s.at[n], s.norm_r.at[n], left).start()

    def send_right(s, n, rows):
        remote(rows, rows, s.right_s.at[n], s.norm_r.at[n], right).start()

    def finish_sum(s, n, owner, place):
        at = place % ring
        own_sum(s, n, owner, at)

        @pl.when(has_left)
        def _():
            add_inc(s, n, owner, at)

        @pl.when(has_right)
        def _():
            remote(s.inc2.at[at], s.inc2.at[at], s.sum_s.at[n], s.inc2_r.at[n], right).wait_recv()
            acc_ref[...] += s.inc2[at].astype(F32)

        total = resid[place] + (acc_ref[...] + s.bias[...])
        if s.final:
            y_ref[place] = total.astype(BF16)
            return
        resid[place] = total
        rows = s.normed.at[owner, core, at]
        rows[...] = layer_norm(total, s.gain[...], s.shift[...])
        pl.when(has_left)(lambda: send_left(s, n, rows))
        pl.when(has_right)(lambda: send_right(s, n, rows))
        remote(rows, rows, s.mate_s.at[n], s.mate_r.at[n], mate).start()

    def pass_norm(s, n, owner, place):
        rows = s.normed.at[owner, core, place % ring]
        remote(rows, rows, s.left_s.at[n], s.norm_r.at[n], left).wait_recv()
        pl.when((z < owner) & has_left)(lambda: send_left(s, n, rows))
        pl.when((z > owner) & has_right)(lambda: send_right(s, n, rows))
        remote(rows, rows, s.mate_s.at[n], s.mate_r.at[n], mate).start()

    def normed_rows(s, j):
        at = (j // chips) % ring
        for turn in range(chips):
            rows, n = s.normed.at[owner_of(turn, chips), 1 - core, at], (j + turn) % span
            remote(rows, rows, s.mate_s.at[n], s.mate_r.at[n], mate).wait_recv()
        return s.normed[:, :, at].reshape(group_rows, s.normed.shape[-1])

    def release(s, j):
        at = (j // chips) % ring
        for turn in range(chips):
            owner, n = owner_of(turn, chips), (j + turn) % span
            mine = s.part.at[owner, core, at]
            remote(mine, s.other.at[owner, at], s.part_s.at[n], s.part_r.at[n], mate).wait_send()
            pl.when(z != owner)(remote(mine, s.inc.at[owner, at], s.sum_s.at[n], s.inc_r.at[n], left).wait_send)
            if not s.final:
                rows = s.normed.at[owner, core, at]
                pl.when((z <= owner) & has_left)(remote(rows, rows, s.left_s.at[n], s.norm_r.at[n], left).wait_send)
                pl.when((z >= owner) & has_right)(remote(rows, rows, s.right_s.at[n], s.norm_r.at[n], right).wait_send)
                remote(rows, rows, s.mate_s.at[n], s.mate_r.at[n], mate).wait_send()

    def project_out(j):
        pl.when(j >= span)(lambda: release(stage_a, j - span))
        store_part(stage_a, j, x_ref[:, :, j // chips].reshape(group_rows, x_ref.shape[-1]), w_out)

    def mlp(j):
        @pl.when(j == 0)
        def _():
            loads[3].wait()
            loads[4].wait()

        rows = normed_rows(stage_a, j)
        for start, width in col_tiles(w_up.shape[1]):
            tile = jnp.dot(rows, w_up[:, start : start + width], preferred_element_type=F32)
            hidden[:, start : start + width] = jax.nn.gelu(tile + b_up[:, start : start + width], approximate=True).astype(BF16)
        pl.when(j >= span)(lambda: release(stage_b, j - span))
        store_part(stage_b, j, hidden[...], w_down)

    def qkv_copy(place):
        return pltpu.make_async_copy(qkv_buf.at[place % 2], qkv_hbm.at[:, :, place], qkv_s.at[place % 2])

    def project_qkv(j):
        place = j // chips
        pl.when(j == 0)(lambda: loads[5].wait())
        pl.when(place >= 2)(lambda: qkv_copy(place - 2).wait())
        rows = normed_rows(stage_b, j)
        for start, width in col_tiles(w_qkv.shape[1]):
            tile = jnp.dot(rows, w_qkv[:, start : start + width], preferred_element_type=F32)
            qkv_buf[place % 2, :, :, :, start : start + width] = tile.astype(BF16).reshape(chips, 2, CHUNK, width)
        qkv_copy(place).start()

    def at_distance(s, j, distance, step):
        inside = (j >= 0) & (j < n_chunks)
        safe = jnp.clip(j, 0, n_chunks - 1)
        owner, place = chunk_place(safe, chips)
        pl.when(inside & (jnp.abs(z - owner) == distance))(lambda: step(s, safe % span, owner, place))

    def at_group(j, step):
        pl.when((j >= 0) & (j < n_chunks) & (j % chips == 0))(lambda: step(jnp.clip(j, 0, n_chunks - chips)))

    def tick(t, carry):
        for s in (stage_b, stage_a):
            for distance in range(far, -1, -1):
                at_distance(s, t - s.start - AHEAD - HOP * (far - distance), distance, finish_sum if distance == 0 else pass_sum)
            if not s.final:
                for distance in range(1, chips):
                    at_distance(s, t - s.start - AHEAD - HOP * (far + distance), distance, pass_norm)
        if not final:
            at_group(t - 2 * span, project_qkv)
        at_group(t - span, mlp)
        at_group(t, project_out)
        return carry

    ticks = span + n_chunks + AHEAD + HOP * far if final else 2 * span + n_chunks - chips + 1
    lax.fori_loop(0, ticks, tick, 0)

    def drain(i, carry):
        release(stage_a, n_chunks - span + i * chips)
        release(stage_b, n_chunks - span + i * chips)
        return carry

    lax.fori_loop(0, ring, drain, 0)
    if not final:
        qkv_copy(per_core - 2).wait()
        qkv_copy(per_core - 1).wait()


def layer_tail(chips, layer, x, resid, w_out, w_up, w_down, bias_a, norm_a, b_up, bias_b, norm_b=None, w_qkv=None):
    seq_len, depth = x.shape
    own, width = resid.shape
    mid = w_up.shape[2]
    per_core = own // CHUNK
    final = norm_b is None
    span = AHEAD + 2 * HOP * (chips - 1) + chips
    ring = span // chips
    assert span % chips == 0 and per_core >= ring
    blocks = (chips, 2, per_core, CHUNK)
    any_spec = pl.BlockSpec(memory_space=pl.ANY)
    vmem = pl.BlockSpec(memory_space=pltpu.VMEM)
    operands = [x.reshape(*blocks, depth), resid.reshape(per_core, CHUNK, width), w_out, w_up, w_down,
                bias_a[None], norm_a[0][None], norm_a[1][None], b_up[None], bias_b[None]]
    in_specs = [any_spec] * 5 + [vmem] * 5
    sems = [pltpu.SemaphoreType.DMA((span,))]
    slots = [
        pltpu.VMEM((chips, 2, ring, CHUNK, width), BF16),
        pltpu.VMEM((chips, ring, CHUNK, width), BF16),
        pltpu.VMEM((chips, ring, CHUNK, width), BF16),
        pltpu.VMEM((ring, CHUNK, width), BF16),
    ]
    norm_slots = [pltpu.VMEM((chips, 2, ring, CHUNK, width), BF16)]
    scratch = [
        pltpu.VMEM((*blocks, depth), BF16),
        pltpu.VMEM((depth, width), BF16),
        pltpu.VMEM((width, mid), BF16),
        pltpu.VMEM((mid, width), BF16),
        pltpu.VMEM((chips * 2 * CHUNK, mid), BF16),
        pltpu.VMEM((CHUNK, width), F32),
        pltpu.SemaphoreType.DMA((6,)),
    ] + slots + norm_slots + sems * 10
    flops = 2 * seq_len * width * (depth + 2 * mid)
    if final:
        out_shape = jax.ShapeDtypeStruct((per_core, CHUNK, width), BF16)
        out_specs = vmem
        scratch += slots + sems * 5 + [pltpu.VMEM((per_core, CHUNK, width), F32)]
    else:
        width2 = w_qkv.shape[1]
        operands += [w_qkv, norm_b[0][None], norm_b[1][None]]
        in_specs += [any_spec, vmem, vmem]
        out_shape = (jax.ShapeDtypeStruct((*blocks, width2), BF16), jax.ShapeDtypeStruct((per_core, CHUNK, width), F32))
        out_specs = (any_spec, vmem)
        scratch += slots + norm_slots + sems * 10
        scratch += [pltpu.VMEM((width, width2), BF16), pltpu.VMEM((2, chips, 2, CHUNK, width2), BF16), pltpu.SemaphoreType.DMA((2,))]
        flops += 2 * seq_len * width * width2
    result = pl.pallas_call(
        functools.partial(layer_kernel, chips, per_core, span, layer, final),
        out_shape=out_shape,
        in_specs=in_specs,
        out_specs=out_specs,
        scratch_shapes=scratch,
        compiler_params=pltpu.CompilerParams(collective_id=layer, has_side_effects=True, vmem_limit_bytes=67043328),
        cost_estimate=pl.CostEstimate(flops=flops, bytes_accessed=40 << 20, transcendentals=0),
        name=f"layer{layer}",
    )(*operands)
    if final:
        return result.reshape(own, width)
    return result[0].reshape(seq_len, width2), result[1].reshape(own, width)


def attention_kernel(scale, block, step, q_ref, k_ref, v_ref, o_ref):
    seq_len = q_ref.shape[0]
    slope = scale * math.log2(math.e)
    last = (((1,), (1,)), ((), ()))
    first = (((0,), (0,)), ((), ()))
    key = lax.broadcasted_iota(jnp.int32, (step, block), 0)
    query = lax.broadcasted_iota(jnp.int32, (step, block), 1)

    def weigh(start, end, probs):
        return lax.dot_general(v_ref[start:end], probs.astype(BF16), first, preferred_element_type=F32)

    def update(whole, skip, new, combine):
        if whole is None:
            return new
        if skip == 0:
            return combine(whole, new)
        return jnp.concatenate([whole[:, :skip], combine(whole[:, skip:], new)], axis=1)

    for start in range(0, seq_len, block):
        q = q_ref[start : start + block]
        top = past = total = out = None
        near = []
        for skip in range(0, block, step):
            keys = k_ref[start + skip : start + skip + step]
            scores = lax.dot_general(keys, q[skip:], last, preferred_element_type=F32)
            scores = jnp.where(key[:, : block - skip] <= query[:, : block - skip], scores, -1e30)
            near.append(scores)
            top = update(top, skip, jnp.max(scores, axis=0, keepdims=True), jnp.maximum)
        if start:
            past = lax.dot_general(k_ref[:start], q, last, preferred_element_type=F32)
            top = jnp.maximum(top, jnp.max(past, axis=0, keepdims=True))
        shift = top * slope
        if start:
            past = jnp.exp2(past * slope - shift)
            total = jnp.sum(past, axis=0, keepdims=True)
            out = weigh(0, start, past)
        for i, skip in enumerate(range(0, block, step)):
            probs = jnp.exp2(near[i] * slope - shift[:, skip:])
            total = update(total, skip, jnp.sum(probs, axis=0, keepdims=True), jnp.add)
            out = update(out, skip, weigh(start + skip, start + skip + step, probs), jnp.add)
        o_ref[start : start + block] = (out / total).astype(BF16).T


def attention(qkv, heads, scale):
    seq_len = qkv.shape[0]
    spec = lambda first: pl.BlockSpec((seq_len, LANES), lambda h: (0, first + h))
    return pl.pallas_call(
        functools.partial(attention_kernel, scale, 1024, 256),
        grid=(heads,),
        out_shape=jax.ShapeDtypeStruct((seq_len, heads * LANES), BF16),
        in_specs=[spec(0), spec(heads), spec(2 * heads)],
        out_specs=spec(0),
        compiler_params=pltpu.CompilerParams(vmem_limit_bytes=60 << 20),
        cost_estimate=pl.CostEstimate(flops=2 * heads * seq_len * seq_len * LANES, bytes_accessed=8 << 20, transcendentals=heads * seq_len * seq_len // 2),
        name="attention",
    )(qkv, qkv, qkv)


def solution(mesh):
    tp_size = mesh.shape["tp"]
    chips = tp_size // 2

    def local_forward(x_local, ln1_gain, ln1_bias, ln2_gain, ln2_bias, w_qkv, w_out, b_out, w_up, b_up, w_down, b_down):
        layers, width, _, heads, head_dim = w_qkv.shape
        scale = 1.0 / math.sqrt(head_dim)
        pad = LANES - head_dim
        wq = jnp.pad(w_qkv, ((0, 0), (0, 0), (0, 0), (0, 0), (0, pad))).reshape(layers, width, 3 * heads * LANES)
        wo = jnp.pad(w_out, ((0, 0), (0, 0), (0, pad), (0, 0))).reshape(layers, heads * LANES, width)
        resid = x_local[0].astype(F32)
        normed = layer_norm(resid, ln1_gain[0], ln1_bias[0])
        gathered = lax.all_gather(normed, "tp", axis=0, tiled=True)
        qkv = jnp.dot(gathered, wq[0], preferred_element_type=F32).astype(BF16)
        for layer in range(layers):
            heads_out = attention(qkv, heads, scale)
            args = (chips, layer, heads_out, resid, wo[layer], w_up, w_down, b_out[layer],
                    (ln2_gain[layer], ln2_bias[layer]), b_up[layer], b_down[layer])
            if layer + 1 < layers:
                qkv, resid = layer_tail(*args, (ln1_gain[layer + 1], ln1_bias[layer + 1]), wq[layer + 1])
            else:
                out = layer_tail(*args)
        return out[None]

    rows_spec = P("dp", "tp", None)
    in_specs = (rows_spec, P(), P(), P(), P(), P(None, None, None, "tp", None), P(None, "tp", None, None), P(), P(None, None, "tp"), P(None, "tp"), P(None, "tp", None), P())
    return jax.shard_map(local_forward, mesh=mesh, in_specs=in_specs, out_specs=rows_spec, check_vma=False)
```

```python
import functools
import math
import jax
import jax.numpy as jnp
from jax import lax
from jax.experimental import pallas as pl
from jax.experimental.pallas import tpu as pltpu
from jax.sharding import PartitionSpec as P

F32 = jnp.float32
BF16 = jnp.bfloat16
LANES = 128
CHUNK = 16
AHEAD = 4
HOP = 4
MESH = pl.DeviceIdType.MESH
LAST = (((1,), (1,)), ((), ()))


def layer_norm(resid, gain, shift):
    row_mean = jnp.mean(resid, axis=-1, keepdims=True)
    centered = resid - row_mean
    variance = jnp.mean(centered * centered, axis=-1, keepdims=True)
    return (centered * lax.rsqrt(variance + 1e-5) * gain + shift).astype(BF16)


def col_tiles(width, tile=512):
    return [(start, min(tile, width - start)) for start in range(0, width, tile)]


def owner_of(turn, chips):
    if isinstance(turn, int):
        return turn // 2 if turn % 2 == 0 else chips - 1 - turn // 2
    return jnp.where(turn % 2 == 0, turn // 2, chips - 1 - turn // 2)


def chunk_place(j, chips):
    return owner_of(j % chips, chips), j // chips


def padded_heads(src, dst):
    heads, head_dim = src.shape[0], src.shape[1]
    return [(src.at[h], dst.at[pl.ds(h * LANES, head_dim)]) for h in range(heads)]


def clear_pads(ref, head_dim):
    for start in range(0, ref.shape[0], LANES):
        ref[start + head_dim : start + LANES] = jnp.zeros((LANES - head_dim, ref.shape[1]), ref.dtype)


def head_kernel(chips, per_core, x_ref, gain, shift, w_qkv_hbm, qkv_hbm, resid, normed, w_qkv, qkv_buf, qkv_s, copy_s,
                norm_r, left_s, right_s, mate_s, mate_r):
    n_chunks = chips * per_core
    far = chips - 1
    heads, head_dim = w_qkv_hbm.shape[2], w_qkv_hbm.shape[3]
    group = lax.axis_index("dp")
    me = lax.axis_index("tp")
    z, core = me // 2, me % 2
    mate = (group, z * 2 + (1 - core))
    left = (group, jnp.maximum(me - 2, 0))
    right = (group, jnp.minimum(me + 2, 2 * chips - 1))
    has_left, has_right = z > 0, z < far

    loads = []
    for part in range(3):
        loads += padded_heads(w_qkv_hbm.at[0, part], w_qkv.at[pl.ds(part * heads * LANES, heads * LANES)])
    loads = [pltpu.make_async_copy(src, dst, copy_s.at[i]) for i, (src, dst) in enumerate(loads)]
    for load in loads:
        load.start()
    clear_pads(w_qkv, head_dim)

    def remote(rows, send, recv, device):
        return pltpu.make_async_remote_copy(src_ref=rows, dst_ref=rows, send_sem=send, recv_sem=recv, device_id=device, device_id_type=MESH)

    barrier = pltpu.get_barrier_semaphore()
    pl.semaphore_signal(barrier, inc=1, device_id=mate, device_id_type=MESH)

    @pl.when(has_left)
    def _():
        pl.semaphore_signal(barrier, inc=1, device_id=left, device_id_type=MESH)

    @pl.when(has_right)
    def _():
        pl.semaphore_signal(barrier, inc=1, device_id=right, device_id_type=MESH)

    pl.semaphore_wait(barrier, 1 + has_left.astype(jnp.int32) + has_right.astype(jnp.int32))

    def to_left(j, rows):
        return remote(rows, left_s.at[j], norm_r.at[j], left)

    def to_right(j, rows):
        return remote(rows, right_s.at[j], norm_r.at[j], right)

    def to_mate(j, rows):
        return remote(rows, mate_s.at[j], mate_r.at[j], mate)

    def own_norm(j, owner, place):
        total = x_ref[place].astype(F32)
        resid[place] = total
        rows = normed.at[owner, core, place]
        rows[...] = layer_norm(total, gain[...], shift[...])
        pl.when(has_left)(lambda: to_left(j, rows).start())
        pl.when(has_right)(lambda: to_right(j, rows).start())
        to_mate(j, rows).start()

    def pass_norm(j, owner, place):
        rows = normed.at[owner, core, place]
        to_left(j, rows).wait_recv()
        pl.when((z < owner) & has_left)(lambda: to_left(j, rows).start())
        pl.when((z > owner) & has_right)(lambda: to_right(j, rows).start())
        to_mate(j, rows).start()

    def qkv_copy(place):
        return pltpu.make_async_copy(qkv_buf.at[place % 2], qkv_hbm.at[:, :, place], qkv_s.at[place % 2])

    def project_qkv(j):
        place = j // chips

        @pl.when(j == 0)
        def _():
            for load in loads:
                load.wait()

        pl.when(place >= 2)(lambda: qkv_copy(place - 2).wait())
        for turn in range(chips):
            to_mate(j + turn, normed.at[owner_of(turn, chips), 1 - core, place]).wait_recv()
        rows = normed[:, :, place].reshape(chips * 2 * CHUNK, normed.shape[-1])
        for start, width in col_tiles(w_qkv.shape[0]):
            tile = lax.dot_general(rows, w_qkv[start : start + width], LAST, preferred_element_type=F32)
            qkv_buf[place % 2, :, :, :, start : start + width] = tile.astype(BF16).reshape(chips, 2, CHUNK, width)
        qkv_copy(place).start()

    def at_distance(j, distance, step):
        inside = (j >= 0) & (j < n_chunks)
        safe = jnp.clip(j, 0, n_chunks - 1)
        owner, place = chunk_place(safe, chips)
        pl.when(inside & (jnp.abs(z - owner) == distance))(lambda: step(safe, owner, place))

    span = HOP * far + chips

    def tick(t, carry):
        for distance in range(chips):
            at_distance(t - HOP * distance, distance, pass_norm if distance else own_norm)
        j = t - span
        pl.when((j >= 0) & (j % chips == 0))(lambda: project_qkv(jnp.clip(j, 0, n_chunks - chips)))
        return carry

    lax.fori_loop(0, span + n_chunks - chips + 1, tick, 0)

    def drain(j, carry):
        owner, place = chunk_place(j, chips)
        rows = normed.at[owner, core, place]
        pl.when((z <= owner) & has_left)(lambda: to_left(j, rows).wait_send())
        pl.when((z >= owner) & has_right)(lambda: to_right(j, rows).wait_send())
        to_mate(j, rows).wait_send()
        return carry

    lax.fori_loop(0, n_chunks, drain, 0)
    qkv_copy(per_core - 2).wait()
    qkv_copy(per_core - 1).wait()


def layer_head(chips, call_id, x, gain, shift, w_qkv):
    own, width = x.shape
    per_core = own // CHUNK
    n_chunks = chips * per_core
    width2 = 3 * w_qkv.shape[2] * LANES
    blocks = (chips, 2, per_core, CHUNK)
    any_spec = pl.BlockSpec(memory_space=pl.ANY)
    vmem = pl.BlockSpec(memory_space=pltpu.VMEM)
    qkv, resid = pl.pallas_call(
        functools.partial(head_kernel, chips, per_core),
        out_shape=(jax.ShapeDtypeStruct((*blocks, width2), BF16), jax.ShapeDtypeStruct((per_core, CHUNK, width), F32)),
        in_specs=[vmem, vmem, vmem, any_spec],
        out_specs=(any_spec, vmem),
        scratch_shapes=[
            pltpu.VMEM((*blocks, width), BF16),
            pltpu.VMEM((width2, width), BF16),
            pltpu.VMEM((2, chips, 2, CHUNK, width2), BF16),
            pltpu.SemaphoreType.DMA((2,)),
            pltpu.SemaphoreType.DMA((3 * w_qkv.shape[2],)),
        ] + [pltpu.SemaphoreType.DMA((n_chunks,))] * 5,
        compiler_params=pltpu.CompilerParams(collective_id=call_id, has_side_effects=True, vmem_limit_bytes=67043328),
        cost_estimate=pl.CostEstimate(flops=2 * 2 * chips * own * width * width2, bytes_accessed=20 << 20, transcendentals=0),
        name="head",
    )(x.reshape(per_core, CHUNK, width), gain[None], shift[None], w_qkv)
    return qkv.reshape(2 * chips * own, width2), resid.reshape(own, width)


class Stage:
    def __init__(self, start, bufs, sems, bias, gain=None, shift=None):
        self.start, self.bias, self.gain, self.shift = start, bias, gain, shift
        self.final = gain is None
        self.part, self.other, self.inc, self.inc2 = bufs[:4]
        self.part_s, self.part_r, self.sum_s, self.inc_r, self.inc2_r = sems[:5]
        if not self.final:
            self.normed = bufs[4]
            self.norm_r, self.left_s, self.right_s, self.mate_s, self.mate_r = sems[5:]


def layer_kernel(chips, per_core, span, layer, final, *refs):
    refs = list(refs)
    take = lambda n: [refs.pop(0) for _ in range(n)]
    x_hbm, resid_hbm, w_out_hbm, w_up_hbm, w_down_hbm, bias_a, gain_a, shift_a, b_up, bias_b = take(10)
    if final:
        (y_ref,) = take(1)
    else:
        w_qkv_hbm, gain_b, shift_b, qkv_hbm, resid = take(5)
    x_ref, w_out, w_up, w_down, hidden, acc_ref, copy_s = take(7)
    stage_a = Stage(0, take(5), take(10), bias_a, gain_a, shift_a)
    if final:
        stage_b = Stage(span, take(4), take(5), bias_b)
        (resid,) = take(1)
    else:
        stage_b = Stage(span, take(5), take(10), bias_b, gain_b, shift_b)
        w_qkv, qkv_buf, qkv_s = take(3)
    n_chunks = chips * per_core
    far = chips - 1
    ring = span // chips
    group_rows = chips * 2 * CHUNK
    group = lax.axis_index("dp")
    me = lax.axis_index("tp")
    z, core = me // 2, me % 2
    mate = (group, z * 2 + (1 - core))
    left = (group, jnp.maximum(me - 2, 0))
    right = (group, jnp.minimum(me + 2, 2 * chips - 1))
    has_left, has_right = z > 0, z < far

    heads = w_out_hbm.shape[1]
    loads = [(x_hbm, x_ref), (resid_hbm, resid)] + padded_heads(w_out_hbm.at[layer], w_out)
    n_first = len(loads)
    loads += [(w_up_hbm.at[layer], w_up), (w_down_hbm.at[layer], w_down)]
    n_mlp = len(loads)
    if not final:
        for part in range(3):
            loads += padded_heads(w_qkv_hbm.at[layer + 1, part], w_qkv.at[pl.ds(part * heads * LANES, heads * LANES)])
    loads = [pltpu.make_async_copy(src, dst, copy_s.at[i]) for i, (src, dst) in enumerate(loads)]
    for load in loads:
        load.start()
    clear_pads(w_out, w_out_hbm.shape[2])
    if not final:
        clear_pads(w_qkv, w_out_hbm.shape[2])

    def remote(src, dst, send, recv, device):
        return pltpu.make_async_remote_copy(src_ref=src, dst_ref=dst, send_sem=send, recv_sem=recv, device_id=device, device_id_type=MESH)

    barrier = pltpu.get_barrier_semaphore()
    pl.semaphore_signal(barrier, inc=1, device_id=mate, device_id_type=MESH)

    @pl.when(has_left)
    def _():
        pl.semaphore_signal(barrier, inc=1, device_id=left, device_id_type=MESH)

    @pl.when(has_right)
    def _():
        pl.semaphore_signal(barrier, inc=1, device_id=right, device_id_type=MESH)

    pl.semaphore_wait(barrier, 1 + has_left.astype(jnp.int32) + has_right.astype(jnp.int32))
    for load in loads[:n_first]:
        load.wait()

    def store_part(s, j, rows, w_ref):
        at = (j // chips) % ring
        for start, width in col_tiles(w_ref.shape[1]):
            tile = jnp.dot(rows, w_ref[:, start : start + width], preferred_element_type=F32)
            s.part[:, :, at, :, start : start + width] = tile.astype(BF16).reshape(chips, 2, CHUNK, width)
        for turn in range(chips):
            owner, n = owner_of(turn, chips), (j + turn) % span
            remote(s.part.at[owner, 1 - core, at], s.other.at[owner, at], s.part_s.at[n], s.part_r.at[n], mate).start()

    def own_sum(s, n, owner, at):
        mine = s.part.at[owner, core, at]
        remote(mine, s.other.at[owner, at], s.part_s.at[n], s.part_r.at[n], mate).wait_recv()
        acc_ref[...] = mine[...].astype(F32) + s.other[owner, at].astype(F32)

    def add_inc(s, n, owner, at):
        remote(s.inc.at[owner, at], s.inc.at[owner, at], s.sum_s.at[n], s.inc_r.at[n], left).wait_recv()
        acc_ref[...] += s.inc[owner, at].astype(F32)

    def pass_sum(s, n, owner, place):
        at = place % ring
        own_sum(s, n, owner, at)

        @pl.when(jnp.where(z < owner, has_left, has_right))
        def _():
            add_inc(s, n, owner, at)

        mine = s.part.at[owner, core, at]
        mine[...] = acc_ref[...].astype(BF16)

        @pl.when(z < owner)
        def _():
            remote(mine, s.inc.at[owner, at], s.sum_s.at[n], s.inc_r.at[n], right).start()

        @pl.when(z > owner + 1)
        def _():
            remote(mine, s.inc.at[owner, at], s.sum_s.at[n], s.inc_r.at[n], left).start()

        @pl.when(z == owner + 1)
        def _():
            remote(mine, s.inc2.at[at], s.sum_s.at[n], s.inc2_r.at[n], left).start()

    def send_left(s, n, rows):
        remote(rows, rows, s.left_s.at[n], s.norm_r.at[n], left).start()

    def send_right(s, n, rows):
        remote(rows, rows, s.right_s.at[n], s.norm_r.at[n], right).start()

    def finish_sum(s, n, owner, place):
        at = place % ring
        own_sum(s, n, owner, at)

        @pl.when(has_left)
        def _():
            add_inc(s, n, owner, at)

        @pl.when(has_right)
        def _():
            remote(s.inc2.at[at], s.inc2.at[at], s.sum_s.at[n], s.inc2_r.at[n], right).wait_recv()
            acc_ref[...] += s.inc2[at].astype(F32)

        total = resid[place] + (acc_ref[...] + s.bias[...])
        if s.final:
            y_ref[place] = total.astype(BF16)
            return
        resid[place] = total
        rows = s.normed.at[owner, core, at]
        rows[...] = layer_norm(total, s.gain[...], s.shift[...])
        pl.when(has_left)(lambda: send_left(s, n, rows))
        pl.when(has_right)(lambda: send_right(s, n, rows))
        remote(rows, rows, s.mate_s.at[n], s.mate_r.at[n], mate).start()

    def pass_norm(s, n, owner, place):
        rows = s.normed.at[owner, core, place % ring]
        remote(rows, rows, s.left_s.at[n], s.norm_r.at[n], left).wait_recv()
        pl.when((z < owner) & has_left)(lambda: send_left(s, n, rows))
        pl.when((z > owner) & has_right)(lambda: send_right(s, n, rows))
        remote(rows, rows, s.mate_s.at[n], s.mate_r.at[n], mate).start()

    def normed_rows(s, j):
        at = (j // chips) % ring
        for turn in range(chips):
            rows, n = s.normed.at[owner_of(turn, chips), 1 - core, at], (j + turn) % span
            remote(rows, rows, s.mate_s.at[n], s.mate_r.at[n], mate).wait_recv()
        return s.normed[:, :, at].reshape(group_rows, s.normed.shape[-1])

    def release(s, j):
        at = (j // chips) % ring
        for turn in range(chips):
            owner, n = owner_of(turn, chips), (j + turn) % span
            mine = s.part.at[owner, core, at]
            remote(mine, s.other.at[owner, at], s.part_s.at[n], s.part_r.at[n], mate).wait_send()
            pl.when(z != owner)(remote(mine, s.inc.at[owner, at], s.sum_s.at[n], s.inc_r.at[n], left).wait_send)
            if not s.final:
                rows = s.normed.at[owner, core, at]
                pl.when((z <= owner) & has_left)(remote(rows, rows, s.left_s.at[n], s.norm_r.at[n], left).wait_send)
                pl.when((z >= owner) & has_right)(remote(rows, rows, s.right_s.at[n], s.norm_r.at[n], right).wait_send)
                remote(rows, rows, s.mate_s.at[n], s.mate_r.at[n], mate).wait_send()

    def project_out(j):
        pl.when(j >= span)(lambda: release(stage_a, j - span))
        store_part(stage_a, j, x_ref[:, :, j // chips].reshape(group_rows, x_ref.shape[-1]), w_out)

    def mlp(j):
        @pl.when(j == 0)
        def _():
            for load in loads[n_first:n_mlp]:
                load.wait()

        rows = normed_rows(stage_a, j)
        for start, width in col_tiles(w_up.shape[1]):
            tile = jnp.dot(rows, w_up[:, start : start + width], preferred_element_type=F32)
            hidden[:, start : start + width] = jax.nn.gelu(tile + b_up[:, start : start + width], approximate=True).astype(BF16)
        pl.when(j >= span)(lambda: release(stage_b, j - span))
        store_part(stage_b, j, hidden[...], w_down)

    def qkv_copy(place):
        return pltpu.make_async_copy(qkv_buf.at[place % 2], qkv_hbm.at[:, :, place], qkv_s.at[place % 2])

    def project_qkv(j):
        place = j // chips

        @pl.when(j == 0)
        def _():
            for load in loads[n_mlp:]:
                load.wait()

        pl.when(place >= 2)(lambda: qkv_copy(place - 2).wait())
        rows = normed_rows(stage_b, j)
        for start, width in col_tiles(w_qkv.shape[0]):
            tile = lax.dot_general(rows, w_qkv[start : start + width], LAST, preferred_element_type=F32)
            qkv_buf[place % 2, :, :, :, start : start + width] = tile.astype(BF16).reshape(chips, 2, CHUNK, width)
        qkv_copy(place).start()

    def at_distance(s, j, distance, step):
        inside = (j >= 0) & (j < n_chunks)
        safe = jnp.clip(j, 0, n_chunks - 1)
        owner, place = chunk_place(safe, chips)
        pl.when(inside & (jnp.abs(z - owner) == distance))(lambda: step(s, safe % span, owner, place))

    def at_group(j, step):
        pl.when((j >= 0) & (j < n_chunks) & (j % chips == 0))(lambda: step(jnp.clip(j, 0, n_chunks - chips)))

    def tick(t, carry):
        for s in (stage_b, stage_a):
            for distance in range(far, -1, -1):
                at_distance(s, t - s.start - AHEAD - HOP * (far - distance), distance, finish_sum if distance == 0 else pass_sum)
            if not s.final:
                for distance in range(1, chips):
                    at_distance(s, t - s.start - AHEAD - HOP * (far + distance), distance, pass_norm)
        if not final:
            at_group(t - 2 * span, project_qkv)
        at_group(t - span, mlp)
        at_group(t, project_out)
        return carry

    ticks = span + n_chunks + AHEAD + HOP * far if final else 2 * span + n_chunks - chips + 1
    lax.fori_loop(0, ticks, tick, 0)

    def drain(i, carry):
        release(stage_a, n_chunks - span + i * chips)
        release(stage_b, n_chunks - span + i * chips)
        return carry

    lax.fori_loop(0, ring, drain, 0)
    if not final:
        qkv_copy(per_core - 2).wait()
        qkv_copy(per_core - 1).wait()


def layer_tail(chips, layer, x, resid, w_out, w_up, w_down, bias_a, norm_a, b_up, bias_b, norm_b=None, w_qkv=None):
    seq_len, depth = x.shape
    own, width = resid.shape
    mid = w_up.shape[2]
    per_core = own // CHUNK
    final = norm_b is None
    span = AHEAD + 2 * HOP * (chips - 1) + chips
    ring = span // chips
    assert span % chips == 0 and per_core >= ring
    blocks = (chips, 2, per_core, CHUNK)
    any_spec = pl.BlockSpec(memory_space=pl.ANY)
    vmem = pl.BlockSpec(memory_space=pltpu.VMEM)
    operands = [x.reshape(*blocks, depth), resid.reshape(per_core, CHUNK, width), w_out, w_up, w_down,
                bias_a[None], norm_a[0][None], norm_a[1][None], b_up[None], bias_b[None]]
    in_specs = [any_spec] * 5 + [vmem] * 5
    sems = [pltpu.SemaphoreType.DMA((span,))]
    slots = [
        pltpu.VMEM((chips, 2, ring, CHUNK, width), BF16),
        pltpu.VMEM((chips, ring, CHUNK, width), BF16),
        pltpu.VMEM((chips, ring, CHUNK, width), BF16),
        pltpu.VMEM((ring, CHUNK, width), BF16),
    ]
    norm_slots = [pltpu.VMEM((chips, 2, ring, CHUNK, width), BF16)]
    scratch = [
        pltpu.VMEM((*blocks, depth), BF16),
        pltpu.VMEM((depth, width), BF16),
        pltpu.VMEM((width, mid), BF16),
        pltpu.VMEM((mid, width), BF16),
        pltpu.VMEM((chips * 2 * CHUNK, mid), BF16),
        pltpu.VMEM((CHUNK, width), F32),
        pltpu.SemaphoreType.DMA((4 + 4 * w_out.shape[1],)),
    ] + slots + norm_slots + sems * 10
    flops = 2 * seq_len * width * (depth + 2 * mid)
    if final:
        out_shape = jax.ShapeDtypeStruct((per_core, CHUNK, width), BF16)
        out_specs = vmem
        scratch += slots + sems * 5 + [pltpu.VMEM((per_core, CHUNK, width), F32)]
    else:
        width2 = 3 * w_qkv.shape[2] * LANES
        operands += [w_qkv, norm_b[0][None], norm_b[1][None]]
        in_specs += [any_spec, vmem, vmem]
        out_shape = (jax.ShapeDtypeStruct((*blocks, width2), BF16), jax.ShapeDtypeStruct((per_core, CHUNK, width), F32))
        out_specs = (any_spec, vmem)
        scratch += slots + norm_slots + sems * 10
        scratch += [pltpu.VMEM((width2, width), BF16), pltpu.VMEM((2, chips, 2, CHUNK, width2), BF16), pltpu.SemaphoreType.DMA((2,))]
        flops += 2 * seq_len * width * width2
    result = pl.pallas_call(
        functools.partial(layer_kernel, chips, per_core, span, layer, final),
        out_shape=out_shape,
        in_specs=in_specs,
        out_specs=out_specs,
        scratch_shapes=scratch,
        compiler_params=pltpu.CompilerParams(collective_id=layer, has_side_effects=True, vmem_limit_bytes=67043328),
        cost_estimate=pl.CostEstimate(flops=flops, bytes_accessed=40 << 20, transcendentals=0),
        name=f"layer{layer}",
    )(*operands)
    if final:
        return result.reshape(own, width)
    return result[0].reshape(seq_len, width2), result[1].reshape(own, width)


def attention_kernel(scale, block, step, q_ref, k_ref, v_ref, o_ref):
    seq_len = q_ref.shape[0]
    slope = scale * math.log2(math.e)
    last = (((1,), (1,)), ((), ()))
    first = (((0,), (0,)), ((), ()))
    key = lax.broadcasted_iota(jnp.int32, (step, block), 0)
    query = lax.broadcasted_iota(jnp.int32, (step, block), 1)

    def weigh(start, end, probs):
        return lax.dot_general(v_ref[start:end], probs.astype(BF16), first, preferred_element_type=F32)

    def update(whole, skip, new, combine):
        if whole is None:
            return new
        if skip == 0:
            return combine(whole, new)
        return jnp.concatenate([whole[:, :skip], combine(whole[:, skip:], new)], axis=1)

    for start in range(0, seq_len, block):
        q = q_ref[start : start + block]
        top = past = total = out = None
        near = []
        for skip in range(0, block, step):
            keys = k_ref[start + skip : start + skip + step]
            scores = lax.dot_general(keys, q[skip:], last, preferred_element_type=F32)
            scores = jnp.where(key[:, : block - skip] <= query[:, : block - skip], scores, -1e30)
            near.append(scores)
            top = update(top, skip, jnp.max(scores, axis=0, keepdims=True), jnp.maximum)
        if start:
            past = lax.dot_general(k_ref[:start], q, last, preferred_element_type=F32)
            top = jnp.maximum(top, jnp.max(past, axis=0, keepdims=True))
        shift = top * slope
        if start:
            past = jnp.exp2(past * slope - shift)
            total = jnp.sum(past, axis=0, keepdims=True)
            out = weigh(0, start, past)
        for i, skip in enumerate(range(0, block, step)):
            probs = jnp.exp2(near[i] * slope - shift[:, skip:])
            total = update(total, skip, jnp.sum(probs, axis=0, keepdims=True), jnp.add)
            out = update(out, skip, weigh(start + skip, start + skip + step, probs), jnp.add)
        o_ref[start : start + block] = (out / total).astype(BF16).T


def attention(qkv, heads, scale):
    seq_len = qkv.shape[0]
    spec = lambda first: pl.BlockSpec((seq_len, LANES), lambda h: (0, first + h))
    return pl.pallas_call(
        functools.partial(attention_kernel, scale, 1024, 256),
        grid=(heads,),
        out_shape=jax.ShapeDtypeStruct((seq_len, heads * LANES), BF16),
        in_specs=[spec(0), spec(heads), spec(2 * heads)],
        out_specs=spec(0),
        compiler_params=pltpu.CompilerParams(vmem_limit_bytes=60 << 20),
        cost_estimate=pl.CostEstimate(flops=2 * heads * seq_len * seq_len * LANES, bytes_accessed=8 << 20, transcendentals=heads * seq_len * seq_len // 2),
        name="attention",
    )(qkv, qkv, qkv)


def solution(mesh):
    tp_size = mesh.shape["tp"]
    chips = tp_size // 2

    def local_forward(x_local, ln1_gain, ln1_bias, ln2_gain, ln2_bias, w_qkv, w_out, b_out, w_up, b_up, w_down, b_down):
        layers, width, _, heads, head_dim = w_qkv.shape
        scale = 1.0 / math.sqrt(head_dim)
        w_qkv = jnp.transpose(w_qkv, (0, 2, 3, 4, 1))
        qkv, resid = layer_head(chips, layers, x_local[0], ln1_gain[0], ln1_bias[0], w_qkv)
        for layer in range(layers):
            heads_out = attention(qkv, heads, scale)
            args = (chips, layer, heads_out, resid, w_out, w_up, w_down, b_out[layer],
                    (ln2_gain[layer], ln2_bias[layer]), b_up[layer], b_down[layer])
            if layer + 1 < layers:
                qkv, resid = layer_tail(*args, (ln1_gain[layer + 1], ln1_bias[layer + 1]), w_qkv)
            else:
                out = layer_tail(*args)
        return out[None]

    rows_spec = P("dp", "tp", None)
    in_specs = (rows_spec, P(), P(), P(), P(), P(None, None, None, "tp", None), P(None, "tp", None, None), P(), P(None, None, "tp"), P(None, "tp"), P(None, "tp", None), P())
    return jax.shard_map(local_forward, mesh=mesh, in_specs=in_specs, out_specs=rows_spec, check_vma=False)
```

```python
import functools
import math
import jax
import jax.numpy as jnp
from jax import lax
from jax.experimental import pallas as pl
from jax.experimental.pallas import tpu as pltpu
from jax.sharding import PartitionSpec as P

F32 = jnp.float32
BF16 = jnp.bfloat16
LANES = 128
CHUNK = 16
AHEAD = 4
HOP = 4
MESH = pl.DeviceIdType.MESH
LAST = (((1,), (1,)), ((), ()))


def layer_norm(resid, gain, shift):
    row_mean = jnp.mean(resid, axis=-1, keepdims=True)
    centered = resid - row_mean
    variance = jnp.mean(centered * centered, axis=-1, keepdims=True)
    return (centered * lax.rsqrt(variance + 1e-5) * gain + shift).astype(BF16)


def col_tiles(width, tile=512):
    return [(start, min(tile, width - start)) for start in range(0, width, tile)]


def owner_of(turn, chips):
    if isinstance(turn, int):
        return turn // 2 if turn % 2 == 0 else chips - 1 - turn // 2
    return jnp.where(turn % 2 == 0, turn // 2, chips - 1 - turn // 2)


def chunk_place(j, chips):
    return owner_of(j % chips, chips), j // chips


def row_of(ref, row):
    return ref[row : row + 1]


def padded_heads(src, dst):
    heads, head_dim = src.shape[0], src.shape[1]
    return [(src.at[h], dst.at[pl.ds(h * LANES, head_dim)]) for h in range(heads)]


def clear_pads(ref, head_dim):
    for start in range(0, ref.shape[0], LANES):
        ref[start + head_dim : start + LANES] = jnp.zeros((LANES - head_dim, ref.shape[1]), ref.dtype)


def head_kernel(chips, per_core, x_ref, gain, shift, w_qkv_hbm, qkv_hbm, resid, normed, w_qkv, qkv_buf, qkv_s, copy_s,
                norm_r, left_s, right_s, mate_s, mate_r):
    n_chunks = chips * per_core
    far = chips - 1
    heads, head_dim = w_qkv_hbm.shape[2], w_qkv_hbm.shape[3]
    group = lax.axis_index("dp")
    me = lax.axis_index("tp")
    z, core = me // 2, me % 2
    mate = (group, z * 2 + (1 - core))
    left = (group, jnp.maximum(me - 2, 0))
    right = (group, jnp.minimum(me + 2, 2 * chips - 1))
    has_left, has_right = z > 0, z < far

    loads = []
    for part in range(3):
        loads += padded_heads(w_qkv_hbm.at[0, part], w_qkv.at[pl.ds(part * heads * LANES, heads * LANES)])
    loads = [pltpu.make_async_copy(src, dst, copy_s.at[i]) for i, (src, dst) in enumerate(loads)]
    for load in loads:
        load.start()
    clear_pads(w_qkv, head_dim)

    def remote(rows, send, recv, device):
        return pltpu.make_async_remote_copy(src_ref=rows, dst_ref=rows, send_sem=send, recv_sem=recv, device_id=device, device_id_type=MESH)

    barrier = pltpu.get_barrier_semaphore()
    pl.semaphore_signal(barrier, inc=1, device_id=mate, device_id_type=MESH)

    @pl.when(has_left)
    def _():
        pl.semaphore_signal(barrier, inc=1, device_id=left, device_id_type=MESH)

    @pl.when(has_right)
    def _():
        pl.semaphore_signal(barrier, inc=1, device_id=right, device_id_type=MESH)

    pl.semaphore_wait(barrier, 1 + has_left.astype(jnp.int32) + has_right.astype(jnp.int32))

    def to_left(j, rows):
        return remote(rows, left_s.at[j], norm_r.at[j], left)

    def to_right(j, rows):
        return remote(rows, right_s.at[j], norm_r.at[j], right)

    def to_mate(j, rows):
        return remote(rows, mate_s.at[j], mate_r.at[j], mate)

    def own_norm(j, owner, place):
        total = x_ref[place].astype(F32)
        resid[place] = total
        rows = normed.at[owner, core, place]
        rows[...] = layer_norm(total, row_of(gain, 0), row_of(shift, 0))
        pl.when(has_left)(lambda: to_left(j, rows).start())
        pl.when(has_right)(lambda: to_right(j, rows).start())
        to_mate(j, rows).start()

    def pass_norm(j, owner, place):
        rows = normed.at[owner, core, place]
        to_left(j, rows).wait_recv()
        pl.when((z < owner) & has_left)(lambda: to_left(j, rows).start())
        pl.when((z > owner) & has_right)(lambda: to_right(j, rows).start())
        to_mate(j, rows).start()

    def qkv_copy(place):
        return pltpu.make_async_copy(qkv_buf.at[place % 2], qkv_hbm.at[:, :, place], qkv_s.at[place % 2])

    def project_qkv(j):
        place = j // chips

        @pl.when(j == 0)
        def _():
            for load in loads:
                load.wait()

        pl.when(place >= 2)(lambda: qkv_copy(place - 2).wait())
        for turn in range(chips):
            to_mate(j + turn, normed.at[owner_of(turn, chips), 1 - core, place]).wait_recv()
        rows = normed[:, :, place].reshape(chips * 2 * CHUNK, normed.shape[-1])
        for start, width in col_tiles(w_qkv.shape[0]):
            tile = lax.dot_general(rows, w_qkv[start : start + width], LAST, preferred_element_type=F32)
            qkv_buf[place % 2, :, :, :, start : start + width] = tile.astype(BF16).reshape(chips, 2, CHUNK, width)
        qkv_copy(place).start()

    def at_distance(j, distance, step):
        inside = (j >= 0) & (j < n_chunks)
        safe = jnp.clip(j, 0, n_chunks - 1)
        owner, place = chunk_place(safe, chips)
        pl.when(inside & (jnp.abs(z - owner) == distance))(lambda: step(safe, owner, place))

    span = HOP * far + chips

    def tick(t, carry):
        for distance in range(chips):
            at_distance(t - HOP * distance, distance, pass_norm if distance else own_norm)
        j = t - span
        pl.when((j >= 0) & (j % chips == 0))(lambda: project_qkv(jnp.clip(j, 0, n_chunks - chips)))
        return carry

    lax.fori_loop(0, span + n_chunks - chips + 1, tick, 0)

    def drain(j, carry):
        owner, place = chunk_place(j, chips)
        rows = normed.at[owner, core, place]
        pl.when((z <= owner) & has_left)(lambda: to_left(j, rows).wait_send())
        pl.when((z >= owner) & has_right)(lambda: to_right(j, rows).wait_send())
        to_mate(j, rows).wait_send()
        return carry

    lax.fori_loop(0, n_chunks, drain, 0)
    qkv_copy(per_core - 2).wait()
    qkv_copy(per_core - 1).wait()


def layer_head(chips, call_id, x, gain, shift, w_qkv):
    own, width = x.shape
    per_core = own // CHUNK
    n_chunks = chips * per_core
    width2 = 3 * w_qkv.shape[2] * LANES
    blocks = (chips, 2, per_core, CHUNK)
    any_spec = pl.BlockSpec(memory_space=pl.ANY)
    vmem = pl.BlockSpec(memory_space=pltpu.VMEM)
    qkv, resid = pl.pallas_call(
        functools.partial(head_kernel, chips, per_core),
        out_shape=(jax.ShapeDtypeStruct((*blocks, width2), BF16), jax.ShapeDtypeStruct((per_core, CHUNK, width), F32)),
        in_specs=[vmem, vmem, vmem, any_spec],
        out_specs=(any_spec, vmem),
        scratch_shapes=[
            pltpu.VMEM((*blocks, width), BF16),
            pltpu.VMEM((width2, width), BF16),
            pltpu.VMEM((2, chips, 2, CHUNK, width2), BF16),
            pltpu.SemaphoreType.DMA((2,)),
            pltpu.SemaphoreType.DMA((3 * w_qkv.shape[2],)),
        ] + [pltpu.SemaphoreType.DMA((n_chunks,))] * 5,
        compiler_params=pltpu.CompilerParams(collective_id=call_id, has_side_effects=True, vmem_limit_bytes=67043328),
        cost_estimate=pl.CostEstimate(flops=2 * 2 * chips * own * width * width2, bytes_accessed=20 << 20, transcendentals=0),
        name="head",
    )(x.reshape(per_core, CHUNK, width), gain, shift, w_qkv)
    return qkv.reshape(2 * chips * own, width2), resid.reshape(own, width)


class Stage:
    def __init__(self, start, bufs, sems, bias, gain=None, shift=None):
        self.start, self.bias, self.gain, self.shift = start, bias, gain, shift
        self.final = gain is None
        self.part, self.other, self.inc, self.inc2 = bufs[:4]
        self.part_s, self.part_r, self.sum_s, self.inc_r, self.inc2_r = sems[:5]
        if not self.final:
            self.normed = bufs[4]
            self.norm_r, self.left_s, self.right_s, self.mate_s, self.mate_r = sems[5:]


def layer_kernel(chips, per_core, span, layer, final, *refs):
    refs = list(refs)
    take = lambda n: [refs.pop(0) for _ in range(n)]
    x_hbm, resid_hbm, w_out_hbm, w_up_hbm, w_down_hbm, bias_a, gain_a, shift_a, b_up, bias_b = take(10)
    if final:
        (y_ref,) = take(1)
    else:
        w_qkv_hbm, gain_b, shift_b, qkv_hbm, resid = take(5)
    x_ref, w_out, w_up, w_down, hidden, acc_ref, copy_s = take(7)
    stage_a = Stage(0, take(5), take(10), (bias_a, layer), (gain_a, layer), (shift_a, layer))
    if final:
        stage_b = Stage(span, take(4), take(5), (bias_b, layer))
        (resid,) = take(1)
    else:
        stage_b = Stage(span, take(5), take(10), (bias_b, layer), (gain_b, layer + 1), (shift_b, layer + 1))
        w_qkv, qkv_buf, qkv_s = take(3)
    n_chunks = chips * per_core
    far = chips - 1
    ring = span // chips
    group_rows = chips * 2 * CHUNK
    group = lax.axis_index("dp")
    me = lax.axis_index("tp")
    z, core = me // 2, me % 2
    mate = (group, z * 2 + (1 - core))
    left = (group, jnp.maximum(me - 2, 0))
    right = (group, jnp.minimum(me + 2, 2 * chips - 1))
    has_left, has_right = z > 0, z < far

    heads = w_out_hbm.shape[1]
    loads = [(x_hbm, x_ref), (resid_hbm, resid)] + padded_heads(w_out_hbm.at[layer], w_out)
    n_first = len(loads)
    loads += [(w_up_hbm.at[layer], w_up), (w_down_hbm.at[layer], w_down)]
    n_mlp = len(loads)
    if not final:
        for part in range(3):
            loads += padded_heads(w_qkv_hbm.at[layer + 1, part], w_qkv.at[pl.ds(part * heads * LANES, heads * LANES)])
    loads = [pltpu.make_async_copy(src, dst, copy_s.at[i]) for i, (src, dst) in enumerate(loads)]
    for load in loads:
        load.start()
    clear_pads(w_out, w_out_hbm.shape[2])
    if not final:
        clear_pads(w_qkv, w_out_hbm.shape[2])

    def remote(src, dst, send, recv, device):
        return pltpu.make_async_remote_copy(src_ref=src, dst_ref=dst, send_sem=send, recv_sem=recv, device_id=device, device_id_type=MESH)

    barrier = pltpu.get_barrier_semaphore()
    pl.semaphore_signal(barrier, inc=1, device_id=mate, device_id_type=MESH)

    @pl.when(has_left)
    def _():
        pl.semaphore_signal(barrier, inc=1, device_id=left, device_id_type=MESH)

    @pl.when(has_right)
    def _():
        pl.semaphore_signal(barrier, inc=1, device_id=right, device_id_type=MESH)

    pl.semaphore_wait(barrier, 1 + has_left.astype(jnp.int32) + has_right.astype(jnp.int32))
    for load in loads[:n_first]:
        load.wait()

    def store_part(s, j, rows, w_ref):
        at = (j // chips) % ring
        for start, width in col_tiles(w_ref.shape[1]):
            tile = jnp.dot(rows, w_ref[:, start : start + width], preferred_element_type=F32)
            s.part[:, :, at, :, start : start + width] = tile.astype(BF16).reshape(chips, 2, CHUNK, width)
        for turn in range(chips):
            owner, n = owner_of(turn, chips), (j + turn) % span
            remote(s.part.at[owner, 1 - core, at], s.other.at[owner, at], s.part_s.at[n], s.part_r.at[n], mate).start()

    def own_sum(s, n, owner, at):
        mine = s.part.at[owner, core, at]
        remote(mine, s.other.at[owner, at], s.part_s.at[n], s.part_r.at[n], mate).wait_recv()
        acc_ref[...] = mine[...].astype(F32) + s.other[owner, at].astype(F32)

    def add_inc(s, n, owner, at):
        remote(s.inc.at[owner, at], s.inc.at[owner, at], s.sum_s.at[n], s.inc_r.at[n], left).wait_recv()
        acc_ref[...] += s.inc[owner, at].astype(F32)

    def pass_sum(s, n, owner, place):
        at = place % ring
        own_sum(s, n, owner, at)

        @pl.when(jnp.where(z < owner, has_left, has_right))
        def _():
            add_inc(s, n, owner, at)

        mine = s.part.at[owner, core, at]
        mine[...] = acc_ref[...].astype(BF16)

        @pl.when(z < owner)
        def _():
            remote(mine, s.inc.at[owner, at], s.sum_s.at[n], s.inc_r.at[n], right).start()

        @pl.when(z > owner + 1)
        def _():
            remote(mine, s.inc.at[owner, at], s.sum_s.at[n], s.inc_r.at[n], left).start()

        @pl.when(z == owner + 1)
        def _():
            remote(mine, s.inc2.at[at], s.sum_s.at[n], s.inc2_r.at[n], left).start()

    def send_left(s, n, rows):
        remote(rows, rows, s.left_s.at[n], s.norm_r.at[n], left).start()

    def send_right(s, n, rows):
        remote(rows, rows, s.right_s.at[n], s.norm_r.at[n], right).start()

    def finish_sum(s, n, owner, place):
        at = place % ring
        own_sum(s, n, owner, at)

        @pl.when(has_left)
        def _():
            add_inc(s, n, owner, at)

        @pl.when(has_right)
        def _():
            remote(s.inc2.at[at], s.inc2.at[at], s.sum_s.at[n], s.inc2_r.at[n], right).wait_recv()
            acc_ref[...] += s.inc2[at].astype(F32)

        total = resid[place] + (acc_ref[...] + row_of(*s.bias))
        if s.final:
            y_ref[place] = total.astype(BF16)
            return
        resid[place] = total
        rows = s.normed.at[owner, core, at]
        rows[...] = layer_norm(total, row_of(*s.gain), row_of(*s.shift))
        pl.when(has_left)(lambda: send_left(s, n, rows))
        pl.when(has_right)(lambda: send_right(s, n, rows))
        remote(rows, rows, s.mate_s.at[n], s.mate_r.at[n], mate).start()

    def pass_norm(s, n, owner, place):
        rows = s.normed.at[owner, core, place % ring]
        remote(rows, rows, s.left_s.at[n], s.norm_r.at[n], left).wait_recv()
        pl.when((z < owner) & has_left)(lambda: send_left(s, n, rows))
        pl.when((z > owner) & has_right)(lambda: send_right(s, n, rows))
        remote(rows, rows, s.mate_s.at[n], s.mate_r.at[n], mate).start()

    def normed_rows(s, j):
        at = (j // chips) % ring
        for turn in range(chips):
            rows, n = s.normed.at[owner_of(turn, chips), 1 - core, at], (j + turn) % span
            remote(rows, rows, s.mate_s.at[n], s.mate_r.at[n], mate).wait_recv()
        return s.normed[:, :, at].reshape(group_rows, s.normed.shape[-1])

    def release(s, j):
        at = (j // chips) % ring
        for turn in range(chips):
            owner, n = owner_of(turn, chips), (j + turn) % span
            mine = s.part.at[owner, core, at]
            remote(mine, s.other.at[owner, at], s.part_s.at[n], s.part_r.at[n], mate).wait_send()
            pl.when(z != owner)(remote(mine, s.inc.at[owner, at], s.sum_s.at[n], s.inc_r.at[n], left).wait_send)
            if not s.final:
                rows = s.normed.at[owner, core, at]
                pl.when((z <= owner) & has_left)(remote(rows, rows, s.left_s.at[n], s.norm_r.at[n], left).wait_send)
                pl.when((z >= owner) & has_right)(remote(rows, rows, s.right_s.at[n], s.norm_r.at[n], right).wait_send)
                remote(rows, rows, s.mate_s.at[n], s.mate_r.at[n], mate).wait_send()

    def project_out(j):
        pl.when(j >= span)(lambda: release(stage_a, j - span))
        store_part(stage_a, j, x_ref[:, :, j // chips].reshape(group_rows, x_ref.shape[-1]), w_out)

    def mlp(j):
        @pl.when(j == 0)
        def _():
            for load in loads[n_first:n_mlp]:
                load.wait()

        rows = normed_rows(stage_a, j)
        for start, width in col_tiles(w_up.shape[1]):
            tile = jnp.dot(rows, w_up[:, start : start + width], preferred_element_type=F32)
            hidden[:, start : start + width] = jax.nn.gelu(tile + b_up[layer : layer + 1, start : start + width], approximate=True).astype(BF16)
        pl.when(j >= span)(lambda: release(stage_b, j - span))
        store_part(stage_b, j, hidden[...], w_down)

    def qkv_copy(place):
        return pltpu.make_async_copy(qkv_buf.at[place % 2], qkv_hbm.at[:, :, place], qkv_s.at[place % 2])

    def project_qkv(j):
        place = j // chips

        @pl.when(j == 0)
        def _():
            for load in loads[n_mlp:]:
                load.wait()

        pl.when(place >= 2)(lambda: qkv_copy(place - 2).wait())
        rows = normed_rows(stage_b, j)
        for start, width in col_tiles(w_qkv.shape[0]):
            tile = lax.dot_general(rows, w_qkv[start : start + width], LAST, preferred_element_type=F32)
            qkv_buf[place % 2, :, :, :, start : start + width] = tile.astype(BF16).reshape(chips, 2, CHUNK, width)
        qkv_copy(place).start()

    def at_distance(s, j, distance, step):
        inside = (j >= 0) & (j < n_chunks)
        safe = jnp.clip(j, 0, n_chunks - 1)
        owner, place = chunk_place(safe, chips)
        pl.when(inside & (jnp.abs(z - owner) == distance))(lambda: step(s, safe % span, owner, place))

    def at_group(j, step):
        pl.when((j >= 0) & (j < n_chunks) & (j % chips == 0))(lambda: step(jnp.clip(j, 0, n_chunks - chips)))

    def tick(t, carry):
        for s in (stage_b, stage_a):
            for distance in range(far, -1, -1):
                at_distance(s, t - s.start - AHEAD - HOP * (far - distance), distance, finish_sum if distance == 0 else pass_sum)
            if not s.final:
                for distance in range(1, chips):
                    at_distance(s, t - s.start - AHEAD - HOP * (far + distance), distance, pass_norm)
        if not final:
            at_group(t - 2 * span, project_qkv)
        at_group(t - span, mlp)
        at_group(t, project_out)
        return carry

    ticks = span + n_chunks + AHEAD + HOP * far if final else 2 * span + n_chunks - chips + 1
    lax.fori_loop(0, ticks, tick, 0)

    def drain(i, carry):
        release(stage_a, n_chunks - span + i * chips)
        release(stage_b, n_chunks - span + i * chips)
        return carry

    lax.fori_loop(0, ring, drain, 0)
    if not final:
        qkv_copy(per_core - 2).wait()
        qkv_copy(per_core - 1).wait()


def layer_tail(chips, layer, x, resid, w_out, w_up, w_down, bias_a, norm_a, b_up, bias_b, norm_b=None, w_qkv=None):
    seq_len, depth = x.shape
    own, width = resid.shape
    mid = w_up.shape[2]
    per_core = own // CHUNK
    final = norm_b is None
    span = AHEAD + 2 * HOP * (chips - 1) + chips
    ring = span // chips
    assert span % chips == 0 and per_core >= ring
    blocks = (chips, 2, per_core, CHUNK)
    any_spec = pl.BlockSpec(memory_space=pl.ANY)
    vmem = pl.BlockSpec(memory_space=pltpu.VMEM)
    operands = [x.reshape(*blocks, depth), resid.reshape(per_core, CHUNK, width), w_out, w_up, w_down,
                bias_a, *norm_a, b_up, bias_b]
    in_specs = [any_spec] * 5 + [vmem] * 5
    sems = [pltpu.SemaphoreType.DMA((span,))]
    slots = [
        pltpu.VMEM((chips, 2, ring, CHUNK, width), BF16),
        pltpu.VMEM((chips, ring, CHUNK, width), BF16),
        pltpu.VMEM((chips, ring, CHUNK, width), BF16),
        pltpu.VMEM((ring, CHUNK, width), BF16),
    ]
    norm_slots = [pltpu.VMEM((chips, 2, ring, CHUNK, width), BF16)]
    scratch = [
        pltpu.VMEM((*blocks, depth), BF16),
        pltpu.VMEM((depth, width), BF16),
        pltpu.VMEM((width, mid), BF16),
        pltpu.VMEM((mid, width), BF16),
        pltpu.VMEM((chips * 2 * CHUNK, mid), BF16),
        pltpu.VMEM((CHUNK, width), F32),
        pltpu.SemaphoreType.DMA((4 + 4 * w_out.shape[1],)),
    ] + slots + norm_slots + sems * 10
    flops = 2 * seq_len * width * (depth + 2 * mid)
    if final:
        out_shape = jax.ShapeDtypeStruct((per_core, CHUNK, width), BF16)
        out_specs = vmem
        scratch += slots + sems * 5 + [pltpu.VMEM((per_core, CHUNK, width), F32)]
    else:
        width2 = 3 * w_qkv.shape[2] * LANES
        operands += [w_qkv, *norm_b]
        in_specs += [any_spec, vmem, vmem]
        out_shape = (jax.ShapeDtypeStruct((*blocks, width2), BF16), jax.ShapeDtypeStruct((per_core, CHUNK, width), F32))
        out_specs = (any_spec, vmem)
        scratch += slots + norm_slots + sems * 10
        scratch += [pltpu.VMEM((width2, width), BF16), pltpu.VMEM((2, chips, 2, CHUNK, width2), BF16), pltpu.SemaphoreType.DMA((2,))]
        flops += 2 * seq_len * width * width2
    result = pl.pallas_call(
        functools.partial(layer_kernel, chips, per_core, span, layer, final),
        out_shape=out_shape,
        in_specs=in_specs,
        out_specs=out_specs,
        scratch_shapes=scratch,
        compiler_params=pltpu.CompilerParams(collective_id=layer, has_side_effects=True, vmem_limit_bytes=67043328),
        cost_estimate=pl.CostEstimate(flops=flops, bytes_accessed=40 << 20, transcendentals=0),
        name=f"layer{layer}",
    )(*operands)
    if final:
        return result.reshape(own, width)
    return result[0].reshape(seq_len, width2), result[1].reshape(own, width)


def attention_kernel(scale, block, step, q_ref, k_ref, v_ref, o_ref):
    seq_len = q_ref.shape[0]
    slope = scale * math.log2(math.e)
    last = (((1,), (1,)), ((), ()))
    first = (((0,), (0,)), ((), ()))
    key = lax.broadcasted_iota(jnp.int32, (step, block), 0)
    query = lax.broadcasted_iota(jnp.int32, (step, block), 1)

    def weigh(start, end, probs):
        return lax.dot_general(v_ref[start:end], probs.astype(BF16), first, preferred_element_type=F32)

    def update(whole, skip, new, combine):
        if whole is None:
            return new
        if skip == 0:
            return combine(whole, new)
        return jnp.concatenate([whole[:, :skip], combine(whole[:, skip:], new)], axis=1)

    for start in range(0, seq_len, block):
        q = q_ref[start : start + block]
        top = past = total = out = None
        near = []
        for skip in range(0, block, step):
            keys = k_ref[start + skip : start + skip + step]
            scores = lax.dot_general(keys, q[skip:], last, preferred_element_type=F32)
            scores = jnp.where(key[:, : block - skip] <= query[:, : block - skip], scores, -1e30)
            near.append(scores)
            top = update(top, skip, jnp.max(scores, axis=0, keepdims=True), jnp.maximum)
        if start:
            past = lax.dot_general(k_ref[:start], q, last, preferred_element_type=F32)
            top = jnp.maximum(top, jnp.max(past, axis=0, keepdims=True))
        shift = top * slope
        if start:
            past = jnp.exp2(past * slope - shift)
            total = jnp.sum(past, axis=0, keepdims=True)
            out = weigh(0, start, past)
        for i, skip in enumerate(range(0, block, step)):
            probs = jnp.exp2(near[i] * slope - shift[:, skip:])
            total = update(total, skip, jnp.sum(probs, axis=0, keepdims=True), jnp.add)
            out = update(out, skip, weigh(start + skip, start + skip + step, probs), jnp.add)
        o_ref[start : start + block] = (out / total).astype(BF16).T


def attention(qkv, heads, scale):
    seq_len = qkv.shape[0]
    spec = lambda first: pl.BlockSpec((seq_len, LANES), lambda h: (0, first + h))
    return pl.pallas_call(
        functools.partial(attention_kernel, scale, 1024, 256),
        grid=(heads,),
        out_shape=jax.ShapeDtypeStruct((seq_len, heads * LANES), BF16),
        in_specs=[spec(0), spec(heads), spec(2 * heads)],
        out_specs=spec(0),
        compiler_params=pltpu.CompilerParams(vmem_limit_bytes=60 << 20),
        cost_estimate=pl.CostEstimate(flops=2 * heads * seq_len * seq_len * LANES, bytes_accessed=8 << 20, transcendentals=heads * seq_len * seq_len // 2),
        name="attention",
    )(qkv, qkv, qkv)


def solution(mesh):
    tp_size = mesh.shape["tp"]
    chips = tp_size // 2

    def local_forward(x_local, ln1_gain, ln1_bias, ln2_gain, ln2_bias, w_qkv, w_out, b_out, w_up, b_up, w_down, b_down):
        layers, width, _, heads, head_dim = w_qkv.shape
        scale = 1.0 / math.sqrt(head_dim)
        w_qkv = jnp.transpose(w_qkv, (0, 2, 3, 4, 1))
        qkv, resid = layer_head(chips, layers, x_local[0], ln1_gain, ln1_bias, w_qkv)
        for layer in range(layers):
            heads_out = attention(qkv, heads, scale)
            args = (chips, layer, heads_out, resid, w_out, w_up, w_down, b_out,
                    (ln2_gain, ln2_bias), b_up, b_down)
            if layer + 1 < layers:
                qkv, resid = layer_tail(*args, (ln1_gain, ln1_bias), w_qkv)
            else:
                out = layer_tail(*args)
        return out[None]

    rows_spec = P("dp", "tp", None)
    in_specs = (rows_spec, P(), P(), P(), P(), P(None, None, None, "tp", None), P(None, "tp", None, None), P(), P(None, None, "tp"), P(None, "tp"), P(None, "tp", None), P())
    return jax.shard_map(local_forward, mesh=mesh, in_specs=in_specs, out_specs=rows_spec, check_vma=False)
```
